32 devices in a mesh: blk: 16 (over z, y, x), band: 2 (over core).
Axes of the slice: x: 2, y: 2, z: 4, core: 2. Of those that a mesh axis runs over, the one named last changes fastest.
Arguments:
- disp_fwd: float32 [16, 2, 25, 2048], P('blk', 'band'), may hold values from -6 to 6
- prev_fwd: float32 [16, 2, 25, 2048], P('blk', 'band'), may hold values from -6 to 6
- disp_adj: float32 [16, 2, 25, 2048], P('blk', 'band'), may hold values from -6 to 6
- prev_adj: float32 [16, 2, 25, 2048], P('blk', 'band'), may hold values from -6 to 6
- modulus: float32 [16, 2, 25, 2048], P('blk', 'band'), may hold values from 0.5 to 2
- radius: float32 [16, 2, 25], P('blk', 'band'), may hold values from 256 to 2048
- step_scale: float32 [16, 2, 25], P('blk', 'band'), may hold values from 0.01 to 0.04
- kernel_in: float32 [16, 2, 25, 2048], P('blk', 'band'), may hold values from -6 to 6
- buckets: int32 [16, 2], P('blk', 'band'), may hold values from 0 to 3
- halo_count: int32 [16, 2, 4], P('blk', 'band'), may hold values from 0 to 8, as said below
- blk_nodes: int32 [16, 2, 2, 8], P('blk', 'band'), may hold values from 0 to 24, as said below
- band_nodes: int32 [16, 2, 2, 4], P('blk', 'band'), may hold values from 0 to 24, as said below
Outputs:
- next_fwd: float32 [16, 2, 25, 2048], P('blk', 'band')
- next_adj: float32 [16, 2, 25, 2048], P('blk', 'band')
- kernel_out: float32 [16, 2, 25, 2048], P('blk', 'band')
The draws below stay inside these ranges and needn't reach their ends.
Inputs may be any that keep to these rules, and one draw needn't show every extreme that they name: `halo_count`: entries 0 and 1 count the nodes shared with the blk neighbour below and above, entries 2 and 3 with the band neighbour below and above. A device's count toward a neighbour equals the neighbour's count back; counts toward the outside of the grid are zero; some pair along blk shares 8 nodes and some pair along band 4. Slot k of a device's list toward a blk neighbour and slot k of that neighbour's list back hold copies of one node; slots at or past the count are unused. The 24 ids of one device over blk_nodes and band_nodes are all different. `band_nodes`: slot k of a device's list toward a band neighbour and slot k of that neighbour's list back hold copies of one node; slots at or past the count are unused; ids are different from those of blk_nodes on the same device.
All inputs are finite; a program needn't handle non-finite values.
Results may differ from the reference program's by a relative error of at most 0.0046.
Values sent between devices are 32-bit elements; how exact they have to be, the bound alone decides.
A program may use at most 64 MiB of HBM per device.

```python
import math
import jax
import jax.numpy as jnp
import numpy as np
from jax import lax

MODES = 1024
COEFF = 2048
SAMPLES = 2048
NODES = 25
EL_DEV = 1
SHARED_Z = 4
SHARED_B = 8
GRID_B = 16
GRID_Z = 2
DEPTH = 2


def shuffle(single_key):
    return jax.random.permutation(single_key, EL_DEV * NODES).astype(jnp.int32)


def halo_plan(key):
    blk_key = jax.random.fold_in(key, 101)
    band_key = jax.random.fold_in(key, 202)
    counts_blk = jax.random.randint(jax.random.fold_in(blk_key, 1), (GRID_B - 1, GRID_Z), 1, SHARED_B + 1, dtype=jnp.int32)
    forced_blk = jax.random.randint(jax.random.fold_in(blk_key, 2), (), 0, (GRID_B - 1) * GRID_Z, dtype=jnp.int32)
    counts_blk = counts_blk.reshape(-1).at[forced_blk].set(SHARED_B).reshape(GRID_B - 1, GRID_Z)
    counts_band = jax.random.randint(jax.random.fold_in(band_key, 1), (GRID_B, GRID_Z - 1), 1, SHARED_Z + 1, dtype=jnp.int32)
    forced_band = jax.random.randint(jax.random.fold_in(band_key, 2), (), 0, GRID_B * (GRID_Z - 1), dtype=jnp.int32)
    counts_band = counts_band.reshape(-1).at[forced_band].set(SHARED_Z).reshape(GRID_B, GRID_Z - 1)
    zero_row = jnp.zeros((1, GRID_Z), jnp.int32)
    zero_col = jnp.zeros((GRID_B, 1), jnp.int32)
    lower_blk = jnp.concatenate([zero_row, counts_blk], axis=0)
    upper_blk = jnp.concatenate([counts_blk, zero_row], axis=0)
    lower_band = jnp.concatenate([zero_col, counts_band], axis=1)
    upper_band = jnp.concatenate([counts_band, zero_col], axis=1)
    counts = jnp.stack([lower_blk, upper_blk, lower_band, upper_band], axis=-1)
    perm_keys = jax.random.split(jax.random.fold_in(key, 303), GRID_B * GRID_Z)
    shuffled = jax.vmap(shuffle)(perm_keys)
    blk_lists = shuffled[:, :2 * SHARED_B].reshape(GRID_B, GRID_Z, 2, SHARED_B)
    band_lists = shuffled[:, 2 * SHARED_B:2 * SHARED_B + 2 * SHARED_Z].reshape(GRID_B, GRID_Z, 2, SHARED_Z)
    return (counts, blk_lists, band_lists)


def draw_halo_count(key, part):
    return halo_plan(key)[0]


def draw_blk_nodes(key, part):
    return halo_plan(key)[1]


def draw_band_nodes(key, part):
    return halo_plan(key)[2]


def with_ends(entries, stream_key, low, high):
    shape = entries.shape
    index_at = [jax.random.randint(jax.random.fold_in(stream_key, axis), (), 0, shape[axis]) for axis in range(len(shape))]
    entries = entries.at[tuple(index_at)].set(low)
    longest = shape.index(max(shape))
    index_at[longest] = (index_at[longest] + 1) % shape[longest]
    return entries.at[tuple(index_at)].set(high)


def shard_levels(key, shape, shards, low, top_value):
    def one(dim, blocks):
        heights = jax.random.uniform(jax.random.fold_in(jax.random.fold_in(key, 6), dim), (blocks,), jnp.float32, low / len(shards), top_value / len(shards))
        return jnp.repeat(jnp.exp(heights), shape[dim] // blocks).reshape((-1,) + (1,) * (len(shape) - dim - 1))

    gain = one(*shards[0])
    for cut in shards[1:]:
        gain = gain * one(*cut)
    return gain


def cumulative_ranks(amount, slope):
    loads = [(1 << 20) // math.isqrt(rank ** slope) + 1 for rank in range(1, amount + 1)]
    spread = 1 + sum(loads) // (1 << 30)
    return np.cumsum(np.array([max(1, weight // spread) for weight in loads]))


def ranked(rng, dims, count, slope):
    grid = cumulative_ranks(count, slope)
    lot = jax.random.randint(jax.random.fold_in(rng, 1), dims, 0, int(grid[count - 1]))
    rank = jnp.searchsorted(jnp.asarray(grid, jnp.int32), lot, side="right")
    return jax.random.permutation(jax.random.fold_in(rng, 2), count)[rank].astype(jnp.int32)


def scatter_about(own_key, extent, scale, limit, cuts=(), kind=jnp.bfloat16):
    entries = scale * jax.random.normal(own_key, extent, jnp.float32)
    if cuts:
        entries = entries * shard_levels(own_key, extent, cuts, -0.22, 0.18)
    return jnp.clip(entries, -limit, limit).astype(kind)


def setup_inputs(seed: int = 0) -> dict:
    splits = jax.random.split(jax.random.key(seed), 13)
    disp_fwd = scatter_about(splits[0], (GRID_B, DEPTH, NODES, COEFF), 1.0, 6.0, ((0, 16), (1, 2)), jnp.float32)
    prev_fwd = scatter_about(splits[1], (GRID_B, DEPTH, NODES, COEFF), 1.0, 6.0, ((0, 16), (1, 2)), jnp.float32)
    disp_adj = scatter_about(splits[2], (GRID_B, DEPTH, NODES, COEFF), 1.0, 6.0, ((0, 16), (1, 2)), jnp.float32)
    prev_adj = scatter_about(splits[3], (GRID_B, DEPTH, NODES, COEFF), 1.0, 6.0, ((0, 16), (1, 2)), jnp.float32)
    modulus = jnp.clip(jnp.exp(math.log(2.0) - 1.3862944 * jax.random.uniform(splits[4], (GRID_B, DEPTH, NODES, SAMPLES), jnp.float32) ** shard_levels(splits[4], (GRID_B, DEPTH, NODES, SAMPLES), ((0, 16), (1, 2)), -0.2, 0.2)), 0.5, 2.0)
    radius = jnp.clip(jnp.exp(math.log(2048.0) - 2.0794415 * jax.random.uniform(splits[5], (GRID_B, DEPTH, NODES), jnp.float32) ** shard_levels(splits[5], (GRID_B, DEPTH, NODES), ((0, 16), (1, 2)), -0.2, 0.2)), 256.0, 2048.0)
    step_scale = jnp.clip(jnp.exp(math.log(0.04) - 1.3862944 * jax.random.uniform(splits[6], (GRID_B, DEPTH, NODES), jnp.float32) ** shard_levels(splits[6], (GRID_B, DEPTH, NODES), ((0, 16), (1, 2)), -0.2, 0.2)), 0.01, 0.04)
    kernel_in = scatter_about(splits[7], (GRID_B, DEPTH, NODES, SAMPLES), 1.0, 6.0, ((0, 16), (1, 2)), jnp.float32)
    buckets = with_ends(ranked(splits[8], (GRID_B, DEPTH), 4, 2), jax.random.fold_in(splits[8], 3), 0, 3).astype(jnp.int32)
    halo_count = draw_halo_count(jax.random.fold_in(splits[12], 71), 0)
    blk_nodes = draw_blk_nodes(jax.random.fold_in(splits[12], 71), 0)
    band_nodes = draw_band_nodes(jax.random.fold_in(splits[12], 71), 0)
    return dict(disp_fwd=disp_fwd, prev_fwd=prev_fwd, disp_adj=disp_adj, prev_adj=prev_adj, modulus=modulus, radius=radius, step_scale=step_scale, kernel_in=kernel_in, buckets=buckets, halo_count=halo_count, blk_nodes=blk_nodes, band_nodes=band_nodes)


def gll_tables():
    inner_root = math.sqrt(3.0 / 7.0)
    points = np.array([-1.0, -inner_root, 0.0, inner_root, 1.0])
    weights = np.array([0.1, 49.0 / 90.0, 32.0 / 45.0, 49.0 / 90.0, 0.1])
    legendre = (35.0 * points ** 4 - 30.0 * points ** 2 + 3.0) / 8.0
    derivative = np.zeros((5, 5))
    for target in range(5):
        for source in range(5):
            if target != source:
                derivative[target, source] = legendre[target] / legendre[source] / (points[target] - points[source])
    derivative[0, 0] = -5.0
    derivative[4, 4] = 5.0
    return (jnp.asarray(derivative, jnp.float32), jnp.asarray(np.outer(weights, weights), jnp.float32))

def azimuth_table(mode_total):
    sample_len = 2 * mode_total
    table_shape = (2 * mode_total, sample_len)
    row_ids = lax.broadcasted_iota(jnp.int32, table_shape, 0)
    col_ids = lax.broadcasted_iota(jnp.int32, table_shape, 1)
    quarter = (row_ids >= mode_total).astype(jnp.int32) * (sample_len // 4)
    phase = (row_ids % mode_total * col_ids + quarter) % sample_len
    factor = math.sqrt(2.0 / sample_len)
    return (jnp.cos(phase.astype(jnp.float32) * (2.0 * math.pi / sample_len)) * factor).astype(jnp.bfloat16)

def mode_tops(mode_total):
    return [max(mode_total // 64, 1), max(mode_total // 16, 1), max(mode_total // 4, 1), mode_total]

def mode_mask(buckets, mode_total):
    order_tops = mode_tops(mode_total)
    order_limit = jnp.where(buckets == 0, order_tops[0], jnp.where(buckets == 1, order_tops[1], jnp.where(buckets == 2, order_tops[2], order_tops[3])))
    kept = (jnp.arange(mode_total, dtype=jnp.int32) < order_limit[..., None]).astype(jnp.float32)
    return jnp.concatenate([kept, kept], axis=-1)

def spin(coeffs, inv_radius, mode_orders):
    half_len = mode_orders.shape[0]
    return jnp.concatenate([-mode_orders * coeffs[..., half_len:], mode_orders * coeffs[..., :half_len]], axis=-1) * inv_radius

def unspin(coeffs, inv_radius, mode_orders):
    half_len = mode_orders.shape[0]
    return jnp.concatenate([mode_orders * coeffs[..., half_len:], -mode_orders * coeffs[..., :half_len]], axis=-1) * inv_radius

def field_terms(coeffs, inv_radius, weight, azim_table, derivative):
    element_total = coeffs.shape[0]
    coeff_len = coeffs.shape[-1]
    sample_len = azim_table.shape[1]
    mode_orders = jnp.arange(coeff_len // 2, dtype=jnp.float32)
    physical = jnp.dot(coeffs.astype(jnp.bfloat16).reshape(-1, coeff_len), azim_table, preferred_element_type=jnp.float32).reshape(element_total, 5, 5, sample_len)
    spun_low = spin(coeffs, inv_radius, mode_orders).astype(jnp.bfloat16).reshape(-1, coeff_len)
    azimuthal = jnp.dot(spun_low, azim_table, preferred_element_type=jnp.float32).reshape(element_total, 5, 5, sample_len)
    grad_s = jnp.einsum('ab,ebjk->eajk', derivative, physical, precision=lax.Precision.HIGHEST)
    grad_z = jnp.einsum('ab,eibk->eiak', derivative, physical, precision=lax.Precision.HIGHEST)
    diverge = jnp.einsum('ba,ebjk->eajk', derivative, weight * grad_s, precision=lax.Precision.HIGHEST) + jnp.einsum('ba,eibk->eiak', derivative, weight * grad_z, precision=lax.Precision.HIGHEST)
    contract_dims = (((1,), (1,)), ((), ()))
    back_div = lax.dot_general(diverge.astype(jnp.bfloat16).reshape(-1, sample_len), azim_table, contract_dims, preferred_element_type=jnp.float32).reshape(element_total, 25, coeff_len)
    back_phi = lax.dot_general((weight * azimuthal).astype(jnp.bfloat16).reshape(-1, sample_len), azim_table, contract_dims, preferred_element_type=jnp.float32).reshape(element_total, 25, coeff_len)
    stiff = back_div + unspin(back_phi, inv_radius, mode_orders)
    return (stiff, grad_s, grad_z, azimuthal)

def pick_rows(table, nodes):
    return table[nodes]

def add_rows(target, nodes, values):
    return target.at[nodes].add(values)

def reference(disp_fwd, prev_fwd, disp_adj, prev_adj, modulus, radius, step_scale, kernel_in, buckets, halo_count, blk_nodes, band_nodes):
    derivative, quadrature = gll_tables()
    azim_table = azimuth_table(MODES)

    def column(inputs):
        col_fwd, col_adj, col_mod, col_rad, col_bucket, col_kernel = inputs
        kept = mode_mask(col_bucket, MODES)[:, None, :]
        inv_radius = 1.0 / col_rad[..., None]
        weight = col_mod.reshape(-1, 5, 5, SAMPLES) * quadrature[None, :, :, None]
        stiff_fwd, fwd_s, fwd_z, fwd_p = field_terms(col_fwd * kept, inv_radius, weight, azim_table, derivative)
        stiff_adj, adj_s, adj_z, adj_p = field_terms(col_adj * kept, inv_radius, weight, azim_table, derivative)
        products = fwd_s * adj_s + fwd_z * adj_z + fwd_p * adj_p
        kernel = col_kernel - (quadrature[None, :, :, None] * products).reshape(-1, NODES, SAMPLES)
        return (stiff_fwd * kept, stiff_adj * kept, kernel)
    stiff_fwd, stiff_adj, kernel_out = lax.map(column, (disp_fwd, disp_adj, modulus, radius, buckets, kernel_in))

    def assemble(stiff):
        local = stiff.reshape(GRID_B, GRID_Z, EL_DEV * NODES, COEFF)
        picker = jax.vmap(jax.vmap(pick_rows))
        placer = jax.vmap(jax.vmap(add_rows))
        blk_slots = jnp.arange(SHARED_B, dtype=jnp.int32)
        band_slots = jnp.arange(SHARED_Z, dtype=jnp.int32)
        total = local
        sends = picker(local, blk_nodes[:, :, 1])
        arrived = jnp.concatenate([jnp.zeros_like(sends[:1]), sends[:-1]], axis=0)
        valid = (blk_slots[None, None, :] < halo_count[:, :, 0:1]).astype(jnp.float32)[..., None]
        total = placer(total, blk_nodes[:, :, 0], arrived * valid)
        sends = picker(local, blk_nodes[:, :, 0])
        arrived = jnp.concatenate([sends[1:], jnp.zeros_like(sends[:1])], axis=0)
        valid = (blk_slots[None, None, :] < halo_count[:, :, 1:2]).astype(jnp.float32)[..., None]
        total = placer(total, blk_nodes[:, :, 1], arrived * valid)
        sends = picker(local, band_nodes[:, :, 1])
        arrived = jnp.concatenate([jnp.zeros_like(sends[:, :1]), sends[:, :-1]], axis=1)
        valid = (band_slots[None, None, :] < halo_count[:, :, 2:3]).astype(jnp.float32)[..., None]
        total = placer(total, band_nodes[:, :, 0], arrived * valid)
        sends = picker(local, band_nodes[:, :, 0])
        arrived = jnp.concatenate([sends[:, 1:], jnp.zeros_like(sends[:, :1])], axis=1)
        valid = (band_slots[None, None, :] < halo_count[:, :, 3:4]).astype(jnp.float32)[..., None]
        total = placer(total, band_nodes[:, :, 1], arrived * valid)
        return total.reshape(GRID_B, DEPTH, NODES, COEFF)
    kept_all = mode_mask(buckets, MODES)[:, :, None, :]
    growth = step_scale[..., None]
    next_fwd = kept_all * (2.0 * (disp_fwd * kept_all) - prev_fwd - growth * assemble(stiff_fwd))
    next_adj = kept_all * (2.0 * (disp_adj * kept_all) - prev_adj - growth * assemble(stiff_adj))
    return (next_fwd, next_adj, kernel_out)
```

```python
import functools
import math

import jax
import jax.numpy as jnp
import ml_dtypes
import numpy as np
from jax import lax
from jax.experimental import pallas as pl
from jax.experimental.pallas import tpu as pltpu
from jax.sharding import PartitionSpec as P

MESH = pl.DeviceIdType.MESH
LANES = 128
ORDER = 5


def gll_tables():
    inner_root = math.sqrt(3.0 / 7.0)
    points = np.array([-1.0, -inner_root, 0.0, inner_root, 1.0])
    weights = np.array([0.1, 49.0 / 90.0, 32.0 / 45.0, 49.0 / 90.0, 0.1])
    legendre = (35.0 * points**4 - 30.0 * points**2 + 3.0) / 8.0
    derivative = np.zeros((5, 5))
    for target in range(5):
        for source in range(5):
            if target != source:
                derivative[target, source] = (
                    legendre[target] / legendre[source] / (points[target] - points[source])
                )
    derivative[0, 0] = -5.0
    derivative[4, 4] = 5.0
    return derivative.astype(np.float32), np.outer(weights, weights).astype(np.float32)


def split_bf16(value):
    high = value.astype(np.float32).astype(ml_dtypes.bfloat16)
    low = (value.astype(np.float32) - high.astype(np.float32)).astype(ml_dtypes.bfloat16)
    return high, low


def stage_tables(tiles):
    total = tiles * LANES
    group = LANES // tiles
    eye = np.eye(group)
    angle = 2.0 * math.pi * np.outer(np.arange(tiles), np.arange(tiles // 2)) / tiles
    cos, sin = np.cos(angle), np.sin(angle)
    fold = np.block([[cos, -sin], [sin, cos]])
    first = np.kron(eye, fold)
    last = np.zeros((group, tiles, 2, group, tiles))
    for v in range(group):
        last[v, :, :, v, :] = fold.T.reshape(tiles, 2, tiles)
    last = last.reshape(LANES, 2 * LANES)
    kb = (np.arange(tiles)[None] * group + np.arange(group)[:, None]).reshape(-1)
    angle = 2.0 * math.pi * ((kb[:, None] * np.arange(LANES)[None]) % LANES) / LANES
    wide = np.concatenate([np.cos(angle), -np.sin(angle)], axis=1) * math.sqrt(2.0 / total)
    angle = 2.0 * math.pi * np.outer(np.arange(tiles), np.arange(LANES)) / total
    turn = np.stack([np.cos(angle), np.sin(angle)])
    turn_t = np.tile(turn.transpose(0, 2, 1), (1, 1, group))
    bf16 = ml_dtypes.bfloat16
    return (
        np.concatenate(split_bf16(first), axis=1),
        wide.astype(np.float32).astype(bf16),
        wide.T.astype(np.float32).astype(bf16),
        np.concatenate(split_bf16(last), axis=1),
        np.concatenate([turn.reshape(2 * tiles, LANES), turn_t.reshape(2 * LANES, LANES)]).astype(np.float32),
    )


def mm(lhs, rhs):
    return jnp.dot(lhs, rhs, preferred_element_type=jnp.float32)


def mm_nt(lhs, rhs):
    return lax.dot_general(lhs, rhs, (((1,), (1,)), ((), ())), preferred_element_type=jnp.float32)


def swap_granules(parts, tiles):
    parts = list(parts)
    lane = lax.broadcasted_iota(jnp.int32, parts[0].shape, 1)
    bit = len(parts) // 2
    while bit:
        upper = ((lane // tiles) & bit) != 0
        for a in range(len(parts)):
            if not a & bit:
                one, two = parts[a], parts[a | bit]
                parts[a] = jnp.where(upper, pltpu.roll(two, bit * tiles, 1), one)
                parts[a | bit] = jnp.where(upper, two, pltpu.roll(one, LANES - bit * tiles, 1))
        bit //= 2
    return parts


def along_line(table, line):
    sum0, dif0 = line[0] + line[4], line[0] - line[4]
    sum1, dif1 = line[1] + line[3], line[1] - line[3]
    out = [None] * 5
    for i in range(2):
        even = (
            float(table[i, 0] + table[i, 4]) / 2 * sum0
            + float(table[i, 1] + table[i, 3]) / 2 * sum1
            + float(table[i, 2]) * line[2]
        )
        odd = float(table[i, 0] - table[i, 4]) / 2 * dif0 + float(table[i, 1] - table[i, 3]) / 2 * dif1
        out[i], out[4 - i] = odd + even, odd - even
    out[2] = float(table[2, 0]) * dif0 + float(table[2, 1]) * dif1
    return out


def kernel(
    blk_total,
    band_total,
    nodes,
    tiles,
    disp_fwd_hbm,
    modulus_hbm,
    disp_adj_hbm,
    prev_fwd_hbm,
    prev_adj_hbm,
    kernel_in_hbm,
    radius_hbm,
    bucket_hbm,
    step_hbm,
    counts_hbm,
    blk_nodes_hbm,
    band_nodes_hbm,
    first_hbm,
    wide_hbm,
    wide_t_hbm,
    last_hbm,
    turn_hbm,
    next_fwd,
    next_adj,
    kernel_out,
    held,
    radius,
    bucket,
    step_scale,
    counts,
    blk_nodes,
    band_nodes,
    first,
    wide,
    wide_t,
    last,
    turn,
    ratio,
    physical,
    azimuth,
    grad_s,
    grad_z,
    diverge,
    stiff,
    send,
    recv_fwd,
    recv_adj,
    held_sem,
    small_sem,
    send_sem,
    recv_sem,
):
    group = LANES // tiles
    half = tiles // 2
    recv = (recv_fwd, recv_adj)
    side_slots = [blk_nodes.shape[-1]] * 2 + [band_nodes.shape[-1]] * 2
    side_start = [sum(side_slots[:side]) for side in range(4)]
    slots = sum(side_slots)
    derivative, quadrature = gll_tables()
    quad = [float(value) for value in quadrature.reshape(-1)]

    def fetch(i, source, target, sems):
        return pltpu.make_async_copy(source, target, sems.at[i])

    sources = (disp_fwd_hbm, modulus_hbm, disp_adj_hbm, kernel_in_hbm, prev_fwd_hbm, prev_adj_hbm)
    fetches = [fetch(i, source, held.at[i], held_sem) for i, source in enumerate(sources)]
    disp_fwd, modulus, disp_adj, kernel_in, prev_fwd, prev_adj = (held.at[i] for i in range(6))
    small = [
        fetch(i, source, target, small_sem)
        for i, (source, target) in enumerate(
            (
                (radius_hbm, radius),
                (bucket_hbm, bucket),
                (first_hbm, first),
                (turn_hbm, turn),
                (wide_hbm, wide),
                (wide_t_hbm, wide_t),
                (last_hbm, last),
                (step_hbm, step_scale),
                (counts_hbm, counts),
                (blk_nodes_hbm, blk_nodes),
                (band_nodes_hbm, band_nodes),
            )
        )
    ]
    small[0].start()
    small[1].start()
    fetches[0].start()
    for copy in small[2:4]:
        copy.start()
    fetches[1].start()
    for copy in small[4:]:
        copy.start()
    for copy in fetches[2:]:
        copy.start()

    blk = lax.axis_index("blk")
    band = lax.axis_index("band")
    links = [
        (blk > 0, (blk - 1, band)),
        (blk < blk_total - 1, (blk + 1, band)),
        (band > 0, (blk, band - 1)),
        (band < band_total - 1, (blk, band + 1)),
    ]
    barrier = pltpu.get_barrier_semaphore()
    for here, peer in links:

        @pl.when(here)
        def _():
            pl.semaphore_signal(barrier, inc=1, device_id=peer, device_id_type=MESH)

    def rows(side):
        return pl.ds(side_start[side], side_slots[side])

    def transfer(f, side):
        return pltpu.make_async_remote_copy(
            src_ref=send.at[f, rows(side)],
            dst_ref=recv[f].at[rows(side ^ 1)],
            send_sem=send_sem.at[f, side],
            recv_sem=recv_sem.at[f, side ^ 1],
            device_id=links[side][1],
            device_id_type=MESH,
        )

    def arrival(f, side):
        return pltpu.make_async_remote_copy(
            src_ref=send.at[f, rows(side)],
            dst_ref=recv[f].at[rows(side)],
            send_sem=send_sem.at[f, side],
            recv_sem=recv_sem.at[f, side],
            device_id=links[side][1],
            device_id_type=MESH,
        )

    for side in range(4):

        @pl.when(jnp.logical_not(links[side][0]))
        def _():
            for ref in recv:
                ref[rows(side)] = jnp.zeros((side_slots[side], tiles, LANES), jnp.float32)

    for ref in recv:
        ref[slots] = jnp.zeros((tiles, LANES), jnp.float32)

    small[0].wait()
    small[1].wait()
    level = bucket[...]
    orders = half * LANES
    tops = [max(orders // 64, 1), max(orders // 16, 1), max(orders // 4, 1), orders]
    limit = jnp.where(
        level == 0, tops[0], jnp.where(level == 1, tops[1], jnp.where(level == 2, tops[2], tops[3]))
    )
    m = lax.broadcasted_iota(jnp.int32, (half, LANES), 0) * LANES + lax.broadcasted_iota(
        jnp.int32, (half, LANES), 1
    )
    kept = (m < limit).astype(jnp.float32)
    kept_m = m.astype(jnp.float32) * kept
    kept2 = jnp.concatenate([kept, kept], axis=0)
    inv_radius = 1.0 / radius[0]
    for n in range(nodes):
        ratio[n * half : (n + 1) * half, :] = kept_m * inv_radius[:, n : n + 1]

    def node(ref, n):
        return ref[n * tiles : (n + 1) * tiles, :]

    whole_groups = nodes // group
    rest = list(range(whole_groups * group, nodes))
    batches = [
        [[(n, 0) for n in range(g * group, (g + 1) * group)], [(n, 1) for n in range(g * group, (g + 1) * group)]]
        for g in range(whole_groups)
    ]
    spare = [(n, q) for n in rest for q in range(2)]
    for start in range(0, len(spare), group):
        batches.append([spare[start : start + group]])

    def fill(parts, dtype):
        return parts + [jnp.zeros((tiles, LANES), dtype)] * (group - len(parts))

    def coefficients(disp, n, q):
        value = node(disp, n)
        if q == 0:
            return (value * kept2).astype(jnp.bfloat16)
        scale = ratio[n * half : (n + 1) * half, :]
        return jnp.concatenate([value[half:] * -scale, value[:half] * scale], axis=0).astype(jnp.bfloat16)

    def to_samples(f, disp, batch):
        blocks = [
            jnp.concatenate(fill([coefficients(disp, n, q) for n, q in part], jnp.bfloat16), axis=0)
            for part in batch
        ]
        rhs = jnp.concatenate(blocks, axis=1)
        count = max(len(part) for part in batch)
        folded = mm(first[: count * 2 * tiles, :], jnp.concatenate([rhs, rhs], axis=0))
        turned = []
        for b, part in enumerate(batch):
            pieces = []
            for v in range(len(part)):
                at = v * 2 * tiles
                re = folded[at : at + tiles, b * LANES : (b + 1) * LANES]
                im = folded[at + tiles : at + 2 * tiles, b * LANES : (b + 1) * LANES]
                cos, sin = turn[:tiles, :], turn[tiles : 2 * tiles, :]
                pieces.append(
                    jnp.concatenate([re * cos - im * sin, re * sin + im * cos], axis=1).astype(jnp.bfloat16)
                )
            pieces += [jnp.zeros((tiles, 2 * LANES), jnp.bfloat16)] * (group - len(pieces))
            turned.append(jnp.concatenate(pieces, axis=0))
        result = mm_nt(wide[...], jnp.concatenate(turned, axis=0))
        for b, part in enumerate(batch):
            spread = [
                result[g * tiles : (g + 1) * tiles, b * LANES : (b + 1) * LANES] for g in range(group)
            ]
            for (n, q), value in zip(part, swap_granules(spread, tiles)):
                (physical, azimuth.at[f])[q][n * tiles : (n + 1) * tiles, :] = value

    def mix(f):
        for j in range(ORDER):
            line = [ORDER * i + j for i in range(ORDER)]
            grads = along_line(derivative, [node(physical, n) for n in line])
            flux = []
            for n, value in zip(line, grads):
                grad_s[f, n * tiles : (n + 1) * tiles, :] = value
                flux.append(node(modulus, n) * quad[n] * value)
            for n, value in zip(line, along_line(derivative.T, flux)):
                diverge[n * tiles : (n + 1) * tiles, :] = value
        for i in range(ORDER):
            line = [ORDER * i + j for j in range(ORDER)]
            grads = along_line(derivative, [node(physical, n) for n in line])
            flux = []
            for n, value in zip(line, grads):
                grad_z[f, n * tiles : (n + 1) * tiles, :] = value
                flux.append(node(modulus, n) * quad[n] * value)
            for n, value in zip(line, along_line(derivative.T, flux)):
                diverge[n * tiles : (n + 1) * tiles, :] += value

    def stress(f, n, q):
        if q == 0:
            return node(diverge, n)
        return node(modulus, n) * quad[n] * node(azimuth.at[f], n)

    def to_stiff(f, batch):
        blocks = []
        for part in batch:
            parts = fill([stress(f, n, q) for n, q in part], jnp.float32)
            blocks.append(jnp.concatenate(swap_granules(parts, tiles), axis=0).astype(jnp.bfloat16))
        spread = mm(wide_t[...], jnp.concatenate(blocks, axis=1))
        cos, sin = turn[2 * tiles : 2 * tiles + LANES, :], turn[2 * tiles + LANES :, :]
        turned = []
        for b in range(len(batch)):
            re = spread[:LANES, b * LANES : (b + 1) * LANES]
            im = spread[LANES:, b * LANES : (b + 1) * LANES]
            turned.append(jnp.concatenate([re * cos + im * sin, im * cos - re * sin], axis=1).astype(jnp.bfloat16))
        rhs = jnp.concatenate(turned, axis=0)
        count = max(len(part) for part in batch)
        back = mm_nt(last[: count * tiles, :], jnp.concatenate([rhs, rhs], axis=1))
        found = {
            entry: back[v * tiles : (v + 1) * tiles, b * LANES : (b + 1) * LANES]
            for b, part in enumerate(batch)
            for v, entry in enumerate(part)
        }
        for n in sorted({n for n, _ in found}):
            div, phi = found[n, 0], found[n, 1]
            scale = ratio[n * half : (n + 1) * half, :]
            stiff[f, n, :half, :] = kept * div[:half] + scale * phi[half:]
            stiff[f, n, half:, :] = kept * div[half:] - scale * phi[:half]

    fields = ((disp_fwd, prev_fwd, next_fwd), (disp_adj, prev_adj, next_adj))
    for f, (disp, _, _) in enumerate(fields):
        if f == 0:
            fetches[0].wait()
            for copy in small[2:]:
                copy.wait()
        else:
            fetches[2].wait()
        for batch in batches:
            to_samples(f, disp, batch)
        if f == 0:
            fetches[1].wait()
        mix(f)
        for batch in batches:
            to_stiff(f, batch)
        if f == 0:
            pl.semaphore_wait(barrier, sum(here.astype(jnp.int32) for here, _ in links))
        for side in range(4):
            lists = blk_nodes if side < 2 else band_nodes
            for s in range(side_slots[side]):
                send[f, side_start[side] + s] = stiff[f, lists[0, 0, side % 2, s]]

            @pl.when(links[side][0])
            def _():
                transfer(f, side).start()

    owners = [
        jnp.where(s < counts[0, 0, side], (blk_nodes, band_nodes)[side // 2][0, 0, side % 2, s], -1)
        for side in range(4)
        for s in range(side_slots[side])
    ]
    slot_of = []
    for n in range(nodes):
        found = jnp.int32(slots)
        for s, owner in enumerate(owners):
            found = jnp.where(owner == n, s, found)
        slot_of.append(found)

    fetches[3].wait()
    for n in range(nodes):
        product = (
            node(grad_s.at[0], n) * node(grad_s.at[1], n)
            + node(grad_z.at[0], n) * node(grad_z.at[1], n)
            + node(azimuth.at[0], n) * node(azimuth.at[1], n)
        )
        kernel_out[n * tiles : (n + 1) * tiles, :] = node(kernel_in, n) - quad[n] * product

    fetches[4].wait()
    fetches[5].wait()
    for f, (disp, prev, out) in enumerate(fields):
        for n in range(nodes):
            now = node(disp, n)
            value = now + now - node(prev, n) - step_scale[0, 0, n] * stiff[f, n]
            out[n * tiles : (n + 1) * tiles, :] = kept2 * value

    for f, (_, _, out) in enumerate(fields):
        for side in range(4):

            @pl.when(links[side][0])
            def _():
                arrival(f, side).wait_recv()

        for n in range(nodes):
            out[n * tiles : (n + 1) * tiles, :] -= kept2 * step_scale[0, 0, n] * recv[f][slot_of[n]]
    for f in range(2):
        for side in range(4):

            @pl.when(links[side][0])
            def _():
                transfer(f, side).wait_send()


def deliver(one, two, three, one_out, two_out, three_out, sems):
    copies = [
        pltpu.make_async_copy(source, target, sems.at[i])
        for i, (source, target) in enumerate(((one, one_out), (two, two_out), (three, three_out)))
    ]
    for copy in copies:
        copy.start()
    for copy in copies:
        copy.wait()


def per_device(
    blk_total,
    band_total,
    disp_fwd,
    prev_fwd,
    disp_adj,
    prev_adj,
    modulus,
    radius,
    step_scale,
    kernel_in,
    buckets,
    halo_count,
    blk_nodes,
    band_nodes,
):
    nodes, coeff_len = disp_fwd.shape[2:]
    tiles = coeff_len // LANES
    slots = 2 * (blk_nodes.shape[-1] + band_nodes.shape[-1])
    first, wide, wide_t, last, turn = stage_tables(tiles)
    hbm = pl.BlockSpec(memory_space=pltpu.HBM)
    vmem = pl.BlockSpec(memory_space=pltpu.VMEM)
    flat = (nodes * tiles, LANES)
    out = jax.ShapeDtypeStruct(flat, jnp.float32)
    outs = pl.pallas_call(
        functools.partial(kernel, blk_total, band_total, nodes, tiles),
        out_shape=(pltpu.VMEM(flat, jnp.float32),) * 3,
        in_specs=[hbm] * 17,
        out_specs=(vmem,) * 3,
        scratch_shapes=[
            pltpu.VMEM((6, *flat), jnp.float32),
            pltpu.VMEM(radius.shape, jnp.float32),
            pltpu.VMEM(buckets.shape, jnp.int32),
            pltpu.SMEM(step_scale.shape, jnp.float32),
            pltpu.SMEM(halo_count.shape, jnp.int32),
            pltpu.SMEM(blk_nodes.shape, jnp.int32),
            pltpu.SMEM(band_nodes.shape, jnp.int32),
            pltpu.VMEM(first.shape, jnp.bfloat16),
            pltpu.VMEM(wide.shape, jnp.bfloat16),
            pltpu.VMEM(wide_t.shape, jnp.bfloat16),
            pltpu.VMEM(last.shape, jnp.bfloat16),
            pltpu.VMEM(turn.shape, jnp.float32),
            pltpu.VMEM((nodes * tiles // 2, LANES), jnp.float32),
            pltpu.VMEM(flat, jnp.float32),
            pltpu.VMEM((2, *flat), jnp.float32),
            pltpu.VMEM((2, *flat), jnp.float32),
            pltpu.VMEM((2, *flat), jnp.float32),
            pltpu.VMEM(flat, jnp.float32),
            pltpu.VMEM((2, nodes, tiles, LANES), jnp.float32),
            pltpu.VMEM((2, slots, tiles, LANES), jnp.float32),
            pltpu.VMEM((slots + 1, tiles, LANES), jnp.float32),
            pltpu.VMEM((slots + 1, tiles, LANES), jnp.float32),
            pltpu.SemaphoreType.DMA((6,)),
            pltpu.SemaphoreType.DMA((11,)),
            pltpu.SemaphoreType.DMA((2, 4)),
            pltpu.SemaphoreType.DMA((2, 4)),
        ],
        compiler_params=pltpu.CompilerParams(
            collective_id=0,
            has_side_effects=True,
            vmem_limit_bytes=67043328 - 3 * 4 * nodes * coeff_len - 40 * 1024,
        ),
    )(
        disp_fwd.reshape(flat),
        modulus.reshape(flat),
        disp_adj.reshape(flat),
        prev_fwd.reshape(flat),
        prev_adj.reshape(flat),
        kernel_in.reshape(flat),
        radius,
        buckets,
        step_scale,
        halo_count,
        blk_nodes,
        band_nodes,
        jnp.asarray(first),
        jnp.asarray(wide),
        jnp.asarray(wide_t),
        jnp.asarray(last),
        jnp.asarray(turn),
    )
    outs = pl.pallas_call(
        deliver,
        out_shape=(out, out, out),
        in_specs=[vmem] * 3,
        out_specs=(hbm,) * 3,
        scratch_shapes=[pltpu.SemaphoreType.DMA((3,))],
        compiler_params=pltpu.CompilerParams(vmem_limit_bytes=4 * 1024 * 1024),
    )(*outs)
    return tuple(value.reshape(disp_fwd.shape) for value in outs)


def solution(mesh):
    wide = P("blk", "band", None, None)
    line = P("blk", "band", None)
    in_specs = (wide,) * 5 + (line, line, wide, P("blk", "band"), line, wide, wide)
    return jax.shard_map(
        functools.partial(per_device, mesh.shape["blk"], mesh.shape["band"]),
        mesh=mesh,
        in_specs=in_specs,
        out_specs=(wide,) * 3,
        check_vma=False,
    )
```

```python
import functools
import math

import jax
import jax.numpy as jnp
import ml_dtypes
import numpy as np
from jax import lax
from jax.experimental import pallas as pl
from jax.experimental.pallas import tpu as pltpu
from jax.sharding import PartitionSpec as P

MESH = pl.DeviceIdType.MESH
LANES = 128
ORDER = 5


def gll_tables():
    inner_root = math.sqrt(3.0 / 7.0)
    points = np.array([-1.0, -inner_root, 0.0, inner_root, 1.0])
    weights = np.array([0.1, 49.0 / 90.0, 32.0 / 45.0, 49.0 / 90.0, 0.1])
    legendre = (35.0 * points**4 - 30.0 * points**2 + 3.0) / 8.0
    derivative = np.zeros((5, 5))
    for target in range(5):
        for source in range(5):
            if target != source:
                derivative[target, source] = (
                    legendre[target] / legendre[source] / (points[target] - points[source])
                )
    derivative[0, 0] = -5.0
    derivative[4, 4] = 5.0
    return derivative.astype(np.float32), np.outer(weights, weights).astype(np.float32)


def rounded(value):
    return np.asarray(value, np.float32).astype(ml_dtypes.bfloat16)


def best_scale(value):
    levels = np.unique(np.round(np.abs(value), 12))
    factors = 1.0 + np.arange(10000) / 10000.0
    scaled = factors[:, None] * levels[None]
    loss = ((rounded(scaled).astype(np.float64) - scaled) ** 2).sum(axis=1) / factors**2
    return float(factors[np.argmin(loss)])


def stage_tables(tiles):
    total = tiles * LANES
    group = LANES // tiles
    angle = 2.0 * math.pi * np.outer(np.arange(tiles), np.arange(tiles // 2)) / tiles
    cos, sin = np.cos(angle), np.sin(angle)
    fold = np.block([[cos, -sin], [sin, cos]])
    kb = (np.arange(tiles)[None] * group + np.arange(group)[:, None]).reshape(-1)
    angle = 2.0 * math.pi * ((kb[:, None] * np.arange(LANES)[None]) % LANES) / LANES
    wide = np.concatenate([np.cos(angle), -np.sin(angle)], axis=1) * math.sqrt(2.0 / total)
    angle = 2.0 * math.pi * np.outer(np.arange(tiles), np.arange(LANES)) / total
    turn = np.concatenate([np.cos(angle), np.sin(angle)])
    fold_scale, wide_scale = best_scale(fold), best_scale(wide)
    first = rounded(np.tile(fold * fold_scale, (1, group)))
    last = rounded(np.tile(fold.T * fold_scale, (1, group)))
    turn = (turn / (fold_scale * wide_scale)).astype(np.float32)
    return first, last, rounded(wide.T * wide_scale), turn


def mm(lhs, rhs):
    return jnp.dot(lhs, rhs, preferred_element_type=jnp.float32)


def mm_nt(lhs, rhs):
    return lax.dot_general(lhs, rhs, (((1,), (1,)), ((), ())), preferred_element_type=jnp.float32)


def blocks_of(tile, group):
    rows, columns = tile.shape
    lane = lax.broadcasted_iota(jnp.int32, tile.shape, 1) // (columns // group)
    value = tile.astype(jnp.float32)
    parts = [jnp.where(lane == v, value, 0.0).astype(jnp.bfloat16) for v in range(group)]
    return jnp.concatenate(parts, axis=0)


def swap_granules(parts, tiles):
    parts = list(parts)
    lane = lax.broadcasted_iota(jnp.int32, parts[0].shape, 1)
    bit = len(parts) // 2
    while bit:
        upper = ((lane // tiles) & bit) != 0
        for a in range(len(parts)):
            if not a & bit:
                one, two = parts[a], parts[a | bit]
                parts[a] = jnp.where(upper, pltpu.roll(two, bit * tiles, 1), one)
                parts[a | bit] = jnp.where(upper, two, pltpu.roll(one, LANES - bit * tiles, 1))
        bit //= 2
    return parts


def along_line(table, line):
    sum0, dif0 = line[0] + line[4], line[0] - line[4]
    sum1, dif1 = line[1] + line[3], line[1] - line[3]
    out = [None] * 5
    for i in range(2):
        even = (
            float(table[i, 0] + table[i, 4]) / 2 * sum0
            + float(table[i, 1] + table[i, 3]) / 2 * sum1
            + float(table[i, 2]) * line[2]
        )
        odd = float(table[i, 0] - table[i, 4]) / 2 * dif0 + float(table[i, 1] - table[i, 3]) / 2 * dif1
        out[i], out[4 - i] = odd + even, odd - even
    out[2] = float(table[2, 0]) * dif0 + float(table[2, 1]) * dif1
    return out


def kernel(
    blk_total,
    band_total,
    nodes,
    tiles,
    disp_fwd_hbm,
    modulus_hbm,
    disp_adj_hbm,
    prev_fwd_hbm,
    prev_adj_hbm,
    kernel_in_hbm,
    radius_hbm,
    bucket_hbm,
    step_hbm,
    counts_hbm,
    blk_nodes_hbm,
    band_nodes_hbm,
    first_hbm,
    last_hbm,
    wide_hbm,
    turn_hbm,
    next_fwd,
    next_adj,
    kernel_out,
    held,
    radius,
    bucket,
    step_scale,
    counts,
    blk_nodes,
    band_nodes,
    first,
    last,
    wide,
    turn,
    first_blocks,
    last_blocks,
    ratio,
    weight,
    physical,
    azimuth,
    grad_s,
    grad_z,
    diverge,
    stiff,
    send,
    recv_fwd,
    recv_adj,
    held_sem,
    small_sem,
    send_sem,
    recv_sem,
):
    group = LANES // tiles
    half = tiles // 2
    recv = (recv_fwd, recv_adj)
    side_slots = [blk_nodes.shape[-1]] * 2 + [band_nodes.shape[-1]] * 2
    side_start = [sum(side_slots[:side]) for side in range(4)]
    slots = sum(side_slots)
    derivative, quadrature = gll_tables()
    quad = [float(value) for value in quadrature.reshape(-1)]

    def fetch(i, source, target, sems):
        return pltpu.make_async_copy(source, target, sems.at[i])

    sources = (disp_fwd_hbm, modulus_hbm, disp_adj_hbm, kernel_in_hbm, prev_fwd_hbm, prev_adj_hbm)
    fetches = [fetch(i, source, held.at[i], held_sem) for i, source in enumerate(sources)]
    disp_fwd, modulus, disp_adj, kernel_in, prev_fwd, prev_adj = (held.at[i] for i in range(6))
    small = [
        fetch(i, source, target, small_sem)
        for i, (source, target) in enumerate(
            (
                (radius_hbm, radius),
                (bucket_hbm, bucket),
                (first_hbm, first),
                (last_hbm, last),
                (turn_hbm, turn),
                (wide_hbm, wide),
                (step_hbm, step_scale),
                (counts_hbm, counts),
                (blk_nodes_hbm, blk_nodes),
                (band_nodes_hbm, band_nodes),
            )
        )
    ]
    small[0].start()
    small[1].start()
    fetches[0].start()
    for copy in small[2:6]:
        copy.start()
    fetches[1].start()
    for copy in small[6:]:
        copy.start()

    blk = lax.axis_index("blk")
    band = lax.axis_index("band")
    links = [
        (blk > 0, (blk - 1, band)),
        (blk < blk_total - 1, (blk + 1, band)),
        (band > 0, (blk, band - 1)),
        (band < band_total - 1, (blk, band + 1)),
    ]
    early = [links[0][0], links[1][0] & (blk != 1), links[2][0], links[3][0]]
    late = [blk < 0, links[1][0] & (blk == 1)]
    barrier = pltpu.get_barrier_semaphore()
    for here, peer in links:

        @pl.when(here)
        def _():
            pl.semaphore_signal(barrier, inc=1, device_id=peer, device_id_type=MESH)

    def rows(side):
        return pl.ds(side_start[side], side_slots[side])

    def transfer(f, side):
        return pltpu.make_async_remote_copy(
            src_ref=send.at[f, rows(side)],
            dst_ref=recv[f].at[rows(side ^ 1)],
            send_sem=send_sem.at[f, side],
            recv_sem=recv_sem.at[f, side ^ 1],
            device_id=links[side][1],
            device_id_type=MESH,
        )

    def arrival(f, side):
        return pltpu.make_async_remote_copy(
            src_ref=send.at[f, rows(side)],
            dst_ref=recv[f].at[rows(side)],
            send_sem=send_sem.at[f, side],
            recv_sem=recv_sem.at[f, side],
            device_id=links[side][1],
            device_id_type=MESH,
        )

    for side in range(4):

        @pl.when(jnp.logical_not(links[side][0]))
        def _():
            for ref in recv:
                ref[rows(side)] = jnp.zeros((side_slots[side], tiles, LANES), jnp.float32)

    for ref in recv:
        ref[slots] = jnp.zeros((tiles, LANES), jnp.float32)

    small[0].wait()
    small[1].wait()
    level = bucket[...]
    orders = half * LANES
    tops = [max(orders // 64, 1), max(orders // 16, 1), max(orders // 4, 1), orders]
    limit = jnp.where(
        level == 0, tops[0], jnp.where(level == 1, tops[1], jnp.where(level == 2, tops[2], tops[3]))
    )
    m = lax.broadcasted_iota(jnp.int32, (half, LANES), 0) * LANES + lax.broadcasted_iota(
        jnp.int32, (half, LANES), 1
    )
    kept = (m < limit).astype(jnp.float32)
    kept_m = m.astype(jnp.float32) * kept
    kept2 = jnp.concatenate([kept, kept], axis=0)
    inv_radius = 1.0 / radius[0]
    for n in range(nodes):
        ratio[n * half : (n + 1) * half, :] = kept_m * inv_radius[:, n : n + 1]

    def node(ref, n):
        return ref[n * tiles : (n + 1) * tiles, :]

    def put(ref, n, value):
        ref[n * tiles : (n + 1) * tiles, :] = value

    whole = nodes // group * group
    blocks = [[[(n, q) for n in range(g, g + group)] for g in range(0, whole, group)] for q in range(2)]
    spare = [(n, q) for n in range(whole, nodes) for q in range(2)]
    blocks[0] += [spare[g : g + group] for g in range(0, len(spare), group)]
    batches = [[[part] for part in side] for side in blocks]
    back_batches = [[[part] for part in side] for side in blocks]

    def stacked(parts):
        parts = parts + [jnp.zeros(parts[0].shape, parts[0].dtype)] * (group - len(parts))
        return jnp.concatenate(parts, axis=0)

    def spot(result, b, at, size):
        return result[at : at + size, b * LANES : (b + 1) * LANES]

    def coefficients(disp, n, q):
        value = node(disp, n)
        if q == 0:
            return (value * kept2).astype(jnp.bfloat16)
        scale = ratio[n * half : (n + 1) * half, :]
        return jnp.concatenate([value[half:] * -scale, value[:half] * scale], axis=0).astype(jnp.bfloat16)

    def to_samples(f, disp, batch):
        rhs = jnp.concatenate(
            [stacked([coefficients(disp, n, q) for n, q in part]) for part in batch], axis=1
        )
        cos, sin = turn[:tiles, :], turn[tiles:, :]
        folded = mm(first_blocks[: max(len(part) for part in batch) * 2 * tiles, :], rhs)
        turned = []
        for b, part in enumerate(batch):
            for v in range(len(part)):
                re = spot(folded, b, v * 2 * tiles, tiles)
                im = spot(folded, b, (v * 2 + 1) * tiles, tiles)
                turned.append(
                    jnp.concatenate([re * cos - im * sin, re * sin + im * cos], axis=1).astype(jnp.bfloat16)
                )
        result = mm(jnp.concatenate(turned, axis=0), wide[...])
        for at, (n, q) in enumerate(entry for part in batch for entry in part):
            put((physical, azimuth.at[f])[q], n, spot(result, 0, at * tiles, tiles))

    def weights():
        for g in range(0, nodes, group):
            part = list(range(g, min(g + group, nodes)))
            parts = [node(modulus, n) for n in part]
            parts += [jnp.zeros((tiles, LANES), jnp.float32)] * (group - len(part))
            turned = jnp.concatenate(swap_granules(parts, tiles), axis=0).T
            for v, n in enumerate(part):
                put(weight, n, quad[n] * turned[v * tiles : (v + 1) * tiles, :])

    def mix(f):
        for j in range(ORDER):
            line = [ORDER * i + j for i in range(ORDER)]
            grads = along_line(derivative, [node(physical, n) for n in line])
            flux = []
            for n, value in zip(line, grads):
                put(grad_s.at[f], n, value)
                flux.append(node(weight, n) * value)
            for n, value in zip(line, along_line(derivative.T, flux)):
                put(diverge, n, value)
        for i in range(ORDER):
            line = [ORDER * i + j for j in range(ORDER)]
            grads = along_line(derivative, [node(physical, n) for n in line])
            flux = []
            for n, value in zip(line, grads):
                put(grad_z.at[f], n, value)
                flux.append(node(weight, n) * value)
            for n, value in zip(line, along_line(derivative.T, flux)):
                put(diverge, n, node(diverge, n) + value)

    def stress(f, n, q):
        value = node(weight, n) * node(azimuth.at[f], n) if q else node(diverge, n)
        return value.astype(jnp.bfloat16)

    def to_coefficients(f, batch, found):
        entries = [entry for part in batch for entry in part]
        cos, sin = turn[:tiles, :], turn[tiles:, :]
        spread = mm_nt(jnp.concatenate([stress(f, n, q) for n, q in entries], axis=0), wide[...])
        turned = {}
        for at, entry in enumerate(entries):
            re = spot(spread, 0, at * tiles, tiles)
            im = spot(spread, 1, at * tiles, tiles)
            turned[entry] = jnp.concatenate([re * cos + im * sin, im * cos - re * sin], axis=0).astype(
                jnp.bfloat16
            )
        rhs = jnp.concatenate([stacked([turned[entry] for entry in part]) for part in batch], axis=1)
        back = mm(last_blocks[: max(len(part) for part in batch) * tiles, :], rhs)
        for b, part in enumerate(batch):
            for v, entry in enumerate(part):
                found[entry] = spot(back, b, v * tiles, tiles)

    fields = ((disp_fwd, prev_fwd, next_fwd), (disp_adj, prev_adj, next_adj))
    for f, (disp, _, _) in enumerate(fields):
        if f == 0:
            for copy in small[2:]:
                copy.wait()
            first_blocks[...] = blocks_of(first[...], group)
            last_blocks[...] = blocks_of(last[...], group)
            fetches[0].wait()
            fetches[1].wait()
            for copy in fetches[2:]:
                copy.start()
        else:
            fetches[2].wait()
        for batch in batches[0]:
            to_samples(f, disp, batch)
        for batch in batches[1]:
            to_samples(f, disp, batch)
        if f == 0:
            weights()
        found = {}
        for batch in back_batches[1]:
            to_coefficients(f, batch, found)
        mix(f)
        for batch in back_batches[0]:
            to_coefficients(f, batch, found)
        for n in range(nodes):
            div, phi = found[n, 0], found[n, 1]
            scale = ratio[n * half : (n + 1) * half, :]
            stiff[f, n, :half, :] = kept * div[:half] + scale * phi[half:]
            stiff[f, n, half:, :] = kept * div[half:] - scale * phi[:half]
        if f == 0:
            pl.semaphore_wait(barrier, sum(here.astype(jnp.int32) for here, _ in links))
        for side in range(4):
            lists = blk_nodes if side < 2 else band_nodes
            for s in range(side_slots[side]):
                send[f, side_start[side] + s] = stiff[f, lists[0, 0, side % 2, s]]

            @pl.when(early[side])
            def _():
                transfer(f, side).start()

    def follow(f):
        for side in range(2):

            @pl.when(late[side])
            def _():
                transfer(f, side).start()

    follow(0)
    follow(1)
    fetches[3].wait()
    for g in range(0, nodes, group):
        part = list(range(g, min(g + group, nodes)))
        products = [
            quad[n]
            * (
                node(grad_s.at[0], n) * node(grad_s.at[1], n)
                + node(grad_z.at[0], n) * node(grad_z.at[1], n)
                + node(azimuth.at[0], n) * node(azimuth.at[1], n)
            )
            for n in part
        ]
        turned = stacked(products).T
        spread = swap_granules([turned[h * tiles : (h + 1) * tiles, :] for h in range(group)], tiles)
        for n, value in zip(part, spread):
            put(kernel_out, n, node(kernel_in, n) - value)

    fetches[4].wait()
    fetches[5].wait()
    for f, (disp, prev, out) in enumerate(fields):
        for n in range(nodes):
            now = node(disp, n)
            value = now + now - node(prev, n) - step_scale[0, 0, n] * stiff[f, n]
            out[n * tiles : (n + 1) * tiles, :] = kept2 * value

    owners = [
        jnp.where(s < counts[0, 0, side], (blk_nodes, band_nodes)[side // 2][0, 0, side % 2, s], -1)
        for side in range(4)
        for s in range(side_slots[side])
    ]
    slot_of = []
    for n in range(nodes):
        found = jnp.int32(slots)
        for s, owner in enumerate(owners):
            found = jnp.where(owner == n, s, found)
        slot_of.append(found)

    for f, (_, _, out) in enumerate(fields):
        for side in range(4):

            @pl.when(links[side][0])
            def _():
                arrival(f, side).wait_recv()

        for n in range(nodes):
            out[n * tiles : (n + 1) * tiles, :] -= kept2 * step_scale[0, 0, n] * recv[f][slot_of[n]]
    for f in range(2):
        for side in range(4):

            @pl.when(links[side][0])
            def _():
                transfer(f, side).wait_send()


def deliver(one, two, three, one_out, two_out, three_out, sems):
    copies = [
        pltpu.make_async_copy(source, target, sems.at[i])
        for i, (source, target) in enumerate(((one, one_out), (two, two_out), (three, three_out)))
    ]
    for copy in copies:
        copy.start()
    for copy in copies:
        copy.wait()


def per_device(
    blk_total,
    band_total,
    disp_fwd,
    prev_fwd,
    disp_adj,
    prev_adj,
    modulus,
    radius,
    step_scale,
    kernel_in,
    buckets,
    halo_count,
    blk_nodes,
    band_nodes,
):
    nodes, coeff_len = disp_fwd.shape[2:]
    tiles = coeff_len // LANES
    slots = 2 * (blk_nodes.shape[-1] + band_nodes.shape[-1])
    first, last, wide, turn = stage_tables(tiles)
    hbm = pl.BlockSpec(memory_space=pltpu.HBM)
    vmem = pl.BlockSpec(memory_space=pltpu.VMEM)
    flat = (nodes * tiles, LANES)
    out = jax.ShapeDtypeStruct(flat, jnp.float32)
    outs = pl.pallas_call(
        functools.partial(kernel, blk_total, band_total, nodes, tiles),
        out_shape=(pltpu.VMEM(flat, jnp.float32),) * 3,
        in_specs=[hbm] * 16,
        out_specs=(vmem,) * 3,
        scratch_shapes=[
            pltpu.VMEM((6, *flat), jnp.float32),
            pltpu.VMEM(radius.shape, jnp.float32),
            pltpu.VMEM(buckets.shape, jnp.int32),
            pltpu.SMEM(step_scale.shape, jnp.float32),
            pltpu.SMEM(halo_count.shape, jnp.int32),
            pltpu.SMEM(blk_nodes.shape, jnp.int32),
            pltpu.SMEM(band_nodes.shape, jnp.int32),
            pltpu.VMEM(first.shape, jnp.bfloat16),
            pltpu.VMEM(last.shape, jnp.bfloat16),
            pltpu.VMEM(wide.shape, jnp.bfloat16),
            pltpu.VMEM(turn.shape, jnp.float32),
            pltpu.VMEM((2 * LANES, LANES), jnp.bfloat16),
            pltpu.VMEM((LANES, 2 * LANES), jnp.bfloat16),
            pltpu.VMEM((nodes * tiles // 2, LANES), jnp.float32),
            pltpu.VMEM(flat, jnp.float32),
            pltpu.VMEM(flat, jnp.float32),
            pltpu.VMEM((2, *flat), jnp.float32),
            pltpu.VMEM((2, *flat), jnp.float32),
            pltpu.VMEM((2, *flat), jnp.float32),
            pltpu.VMEM(flat, jnp.float32),
            pltpu.VMEM((2, nodes, tiles, LANES), jnp.float32),
            pltpu.VMEM((2, slots, tiles, LANES), jnp.float32),
            pltpu.VMEM((slots + 1, tiles, LANES), jnp.float32),
            pltpu.VMEM((slots + 1, tiles, LANES), jnp.float32),
            pltpu.SemaphoreType.DMA((6,)),
            pltpu.SemaphoreType.DMA((10,)),
            pltpu.SemaphoreType.DMA((2, 4)),
            pltpu.SemaphoreType.DMA((2, 4)),
        ],
        compiler_params=pltpu.CompilerParams(
            collective_id=0,
            has_side_effects=True,
            vmem_limit_bytes=67043328 - 3 * 4 * nodes * coeff_len - 40 * 1024,
        ),
    )(
        disp_fwd.reshape(flat),
        modulus.reshape(flat),
        disp_adj.reshape(flat),
        prev_fwd.reshape(flat),
        prev_adj.reshape(flat),
        kernel_in.reshape(flat),
        radius,
        buckets,
        step_scale,
        halo_count,
        blk_nodes,
        band_nodes,
        jnp.asarray(first),
        jnp.asarray(last),
        jnp.asarray(wide),
        jnp.asarray(turn),
    )
    outs = pl.pallas_call(
        deliver,
        out_shape=(out, out, out),
        in_specs=[vmem] * 3,
        out_specs=(hbm,) * 3,
        scratch_shapes=[pltpu.SemaphoreType.DMA((3,))],
        compiler_params=pltpu.CompilerParams(vmem_limit_bytes=4 * 1024 * 1024),
    )(*outs)
    return tuple(value.reshape(disp_fwd.shape) for value in outs)


def solution(mesh):
    wide = P("blk", "band", None, None)
    line = P("blk", "band", None)
    in_specs = (wide,) * 5 + (line, line, wide, P("blk", "band"), line, wide, wide)
    return jax.shard_map(
        functools.partial(per_device, mesh.shape["blk"], mesh.shape["band"]),
        mesh=mesh,
        in_specs=in_specs,
        out_specs=(wide,) * 3,
        check_vma=False,
    )
```

```python
import functools
import math

import jax
import jax.numpy as jnp
import ml_dtypes
import numpy as np
from jax import lax
from jax.experimental import pallas as pl
from jax.experimental.pallas import tpu as pltpu
from jax.sharding import PartitionSpec as P

MESH = pl.DeviceIdType.MESH
LANES = 128
ORDER = 5


def gll_tables():
    inner_root = math.sqrt(3.0 / 7.0)
    points = np.array([-1.0, -inner_root, 0.0, inner_root, 1.0])
    weights = np.array([0.1, 49.0 / 90.0, 32.0 / 45.0, 49.0 / 90.0, 0.1])
    legendre = (35.0 * points**4 - 30.0 * points**2 + 3.0) / 8.0
    derivative = np.zeros((5, 5))
    for target in range(5):
        for source in range(5):
            if target != source:
                derivative[target, source] = (
                    legendre[target] / legendre[source] / (points[target] - points[source])
                )
    derivative[0, 0] = -5.0
    derivative[4, 4] = 5.0
    return derivative.astype(np.float32), np.outer(weights, weights).astype(np.float32)


def rounded(value):
    return np.asarray(value, np.float32).astype(ml_dtypes.bfloat16)


def best_scale(value):
    levels = np.unique(np.round(np.abs(value), 12))
    factors = 1.0 + np.arange(10000) / 10000.0
    scaled = factors[:, None] * levels[None]
    loss = ((rounded(scaled).astype(np.float64) - scaled) ** 2).sum(axis=1) / factors**2
    return float(factors[np.argmin(loss)])


def stage_tables(tiles):
    total = tiles * LANES
    group = LANES // tiles
    angle = 2.0 * math.pi * np.outer(np.arange(tiles), np.arange(tiles // 2)) / tiles
    cos, sin = np.cos(angle), np.sin(angle)
    fold = np.block([[cos, -sin], [sin, cos]])
    kb = (np.arange(tiles)[None] * group + np.arange(group)[:, None]).reshape(-1)
    angle = 2.0 * math.pi * ((kb[:, None] * np.arange(LANES)[None]) % LANES) / LANES
    wide = np.concatenate([np.cos(angle), -np.sin(angle)], axis=1) * math.sqrt(2.0 / total)
    angle = 2.0 * math.pi * np.outer(np.arange(tiles), np.arange(LANES)) / total
    turn = np.concatenate([np.cos(angle), np.sin(angle)])
    fold_scale, wide_scale = best_scale(fold), best_scale(wide)
    first = rounded(np.tile(fold * fold_scale, (1, group)))
    last = rounded(np.tile(fold.T * fold_scale, (1, group)))
    turn = (turn / (fold_scale * wide_scale)).astype(np.float32)
    return first, last, rounded(wide.T * wide_scale), turn


def mm(lhs, rhs):
    return jnp.dot(lhs, rhs, preferred_element_type=jnp.float32)


def mm_nt(lhs, rhs):
    return lax.dot_general(lhs, rhs, (((1,), (1,)), ((), ())), preferred_element_type=jnp.float32)


def blocks_of(tile, group):
    rows, columns = tile.shape
    lane = lax.broadcasted_iota(jnp.int32, tile.shape, 1) // (columns // group)
    value = tile.astype(jnp.float32)
    parts = [jnp.where(lane == v, value, 0.0).astype(jnp.bfloat16) for v in range(group)]
    return jnp.concatenate(parts, axis=0)


def swap_granules(parts, tiles):
    parts = list(parts)
    lane = lax.broadcasted_iota(jnp.int32, parts[0].shape, 1)
    bit = len(parts) // 2
    while bit:
        upper = ((lane // tiles) & bit) != 0
        for a in range(len(parts)):
            if not a & bit:
                one, two = parts[a], parts[a | bit]
                parts[a] = jnp.where(upper, pltpu.roll(two, bit * tiles, 1), one)
                parts[a | bit] = jnp.where(upper, two, pltpu.roll(one, LANES - bit * tiles, 1))
        bit //= 2
    return parts


def along_line(table, line):
    sum0, dif0 = line[0] + line[4], line[0] - line[4]
    sum1, dif1 = line[1] + line[3], line[1] - line[3]
    out = [None] * 5
    for i in range(2):
        even = (
            float(table[i, 0] + table[i, 4]) / 2 * sum0
            + float(table[i, 1] + table[i, 3]) / 2 * sum1
            + float(table[i, 2]) * line[2]
        )
        odd = float(table[i, 0] - table[i, 4]) / 2 * dif0 + float(table[i, 1] - table[i, 3]) / 2 * dif1
        out[i], out[4 - i] = odd + even, odd - even
    out[2] = float(table[2, 0]) * dif0 + float(table[2, 1]) * dif1
    return out


def kernel(
    blk_total,
    band_total,
    nodes,
    tiles,
    disp_fwd_hbm,
    modulus_hbm,
    disp_adj_hbm,
    prev_fwd_hbm,
    prev_adj_hbm,
    kernel_in_hbm,
    radius_hbm,
    bucket_hbm,
    step_hbm,
    counts_hbm,
    blk_nodes_hbm,
    band_nodes_hbm,
    first_hbm,
    last_hbm,
    wide_hbm,
    turn_hbm,
    next_fwd,
    next_adj,
    kernel_out,
    held,
    radius,
    bucket,
    step_scale,
    counts,
    blk_nodes,
    band_nodes,
    first,
    last,
    wide,
    turn,
    first_blocks,
    last_blocks,
    ratio,
    weight,
    physical,
    azimuth,
    grad_s,
    grad_z,
    diverge,
    stiff,
    send,
    recv_fwd,
    recv_adj,
    held_sem,
    small_sem,
    send_sem,
    recv_sem,
):
    group = LANES // tiles
    half = tiles // 2
    recv = (recv_fwd, recv_adj)
    side_slots = [blk_nodes.shape[-1]] * 2 + [band_nodes.shape[-1]] * 2
    side_start = [sum(side_slots[:side]) for side in range(4)]
    slots = sum(side_slots)
    derivative, quadrature = gll_tables()
    quad = [float(value) for value in quadrature.reshape(-1)]

    def fetch(i, source, target, sems):
        return pltpu.make_async_copy(source, target, sems.at[i])

    sources = (disp_fwd_hbm, modulus_hbm, disp_adj_hbm, kernel_in_hbm, prev_fwd_hbm, prev_adj_hbm)
    fetches = [fetch(i, source, held.at[i], held_sem) for i, source in enumerate(sources)]
    disp_fwd, modulus, disp_adj, kernel_in, prev_fwd, prev_adj = (held.at[i] for i in range(6))
    small = [
        fetch(i, source, target, small_sem)
        for i, (source, target) in enumerate(
            (
                (radius_hbm, radius),
                (bucket_hbm, bucket),
                (first_hbm, first),
                (last_hbm, last),
                (turn_hbm, turn),
                (wide_hbm, wide),
                (step_hbm, step_scale),
                (counts_hbm, counts),
                (blk_nodes_hbm, blk_nodes),
                (band_nodes_hbm, band_nodes),
            )
        )
    ]
    small[0].start()
    small[1].start()
    fetches[0].start()
    for copy in small[2:6]:
        copy.start()
    fetches[1].start()
    for copy in small[6:]:
        copy.start()

    blk = lax.axis_index("blk")
    band = lax.axis_index("band")
    links = [
        (blk > 0, (blk - 1, band)),
        (blk < blk_total - 1, (blk + 1, band)),
        (band > 0, (blk, band - 1)),
        (band < band_total - 1, (blk, band + 1)),
    ]
    early = [links[0][0], links[1][0] & (blk != 1), links[2][0], links[3][0]]
    late = [blk < 0, links[1][0] & (blk == 1)]
    barrier = pltpu.get_barrier_semaphore()
    for here, peer in links:

        @pl.when(here)
        def _():
            pl.semaphore_signal(barrier, inc=1, device_id=peer, device_id_type=MESH)

    def rows(side):
        return pl.ds(side_start[side], side_slots[side])

    def transfer(f, side):
        return pltpu.make_async_remote_copy(
            src_ref=send.at[f, rows(side)],
            dst_ref=recv[f].at[rows(side ^ 1)],
            send_sem=send_sem.at[f, side],
            recv_sem=recv_sem.at[f, side ^ 1],
            device_id=links[side][1],
            device_id_type=MESH,
        )

    def arrival(f, side):
        return pltpu.make_async_remote_copy(
            src_ref=send.at[f, rows(side)],
            dst_ref=recv[f].at[rows(side)],
            send_sem=send_sem.at[f, side],
            recv_sem=recv_sem.at[f, side],
            device_id=links[side][1],
            device_id_type=MESH,
        )

    for side in range(4):

        @pl.when(jnp.logical_not(links[side][0]))
        def _():
            for ref in recv:
                ref[rows(side)] = jnp.zeros((side_slots[side], tiles, LANES), jnp.float32)

    for ref in recv:
        ref[slots] = jnp.zeros((tiles, LANES), jnp.float32)

    small[0].wait()
    small[1].wait()
    level = bucket[...]
    orders = half * LANES
    tops = [max(orders // 64, 1), max(orders // 16, 1), max(orders // 4, 1), orders]
    limit = jnp.where(
        level == 0, tops[0], jnp.where(level == 1, tops[1], jnp.where(level == 2, tops[2], tops[3]))
    )
    m = lax.broadcasted_iota(jnp.int32, (half, LANES), 0) * LANES + lax.broadcasted_iota(
        jnp.int32, (half, LANES), 1
    )
    kept = (m < limit).astype(jnp.float32)
    kept_m = m.astype(jnp.float32) * kept
    kept2 = jnp.concatenate([kept, kept], axis=0)
    inv_radius = 1.0 / radius[0]
    for n in range(nodes):
        ratio[n * half : (n + 1) * half, :] = kept_m * inv_radius[:, n : n + 1]

    def node(ref, n):
        return ref[n * tiles : (n + 1) * tiles, :]

    def put(ref, n, value):
        ref[n * tiles : (n + 1) * tiles, :] = value

    whole = nodes // group * group
    blocks = [[[(n, q) for n in range(g, g + group)] for g in range(0, whole, group)] for q in range(2)]
    spare = [(n, q) for n in range(whole, nodes) for q in range(2)]
    blocks[0] += [spare[g : g + group] for g in range(0, len(spare), group)]
    batches = [[[part] for part in side] for side in blocks]
    back_batches = [[[part] for part in side] for side in blocks]

    def stacked(parts):
        parts = parts + [jnp.zeros(parts[0].shape, parts[0].dtype)] * (group - len(parts))
        return jnp.concatenate(parts, axis=0)

    def spot(result, b, at, size):
        return result[at : at + size, b * LANES : (b + 1) * LANES]

    def coefficients(disp, n, q):
        value = node(disp, n)
        if q == 0:
            return (value * kept2).astype(jnp.bfloat16)
        scale = ratio[n * half : (n + 1) * half, :]
        return jnp.concatenate([value[half:] * -scale, value[:half] * scale], axis=0).astype(jnp.bfloat16)

    def to_samples(f, disp, group_batches):
        folds = []
        for batch in group_batches:
            rhs = jnp.concatenate(
                [stacked([coefficients(disp, n, q) for n, q in part]) for part in batch], axis=1
            )
            folds.append(mm(first_blocks[: max(len(part) for part in batch) * 2 * tiles, :], rhs))
        cos, sin = turn[:tiles, :], turn[tiles:, :]
        for batch, folded in zip(group_batches, folds):
            turned = []
            for b, part in enumerate(batch):
                for v in range(len(part)):
                    re = spot(folded, b, v * 2 * tiles, tiles)
                    im = spot(folded, b, (v * 2 + 1) * tiles, tiles)
                    turned.append(
                        jnp.concatenate([re * cos - im * sin, re * sin + im * cos], axis=1).astype(jnp.bfloat16)
                    )
            result = mm(jnp.concatenate(turned, axis=0), wide[...])
            for at, (n, q) in enumerate(entry for part in batch for entry in part):
                put((physical, azimuth.at[f])[q], n, spot(result, 0, at * tiles, tiles))

    def weights():
        for g in range(0, nodes, group):
            part = list(range(g, min(g + group, nodes)))
            parts = [node(modulus, n) for n in part]
            parts += [jnp.zeros((tiles, LANES), jnp.float32)] * (group - len(part))
            turned = jnp.concatenate(swap_granules(parts, tiles), axis=0).T
            for v, n in enumerate(part):
                put(weight, n, quad[n] * turned[v * tiles : (v + 1) * tiles, :])

    def mix(f):
        for j in range(ORDER):
            line = [ORDER * i + j for i in range(ORDER)]
            grads = along_line(derivative, [node(physical, n) for n in line])
            flux = []
            for n, value in zip(line, grads):
                put(grad_s.at[f], n, value)
                flux.append(node(weight, n) * value)
            for n, value in zip(line, along_line(derivative.T, flux)):
                put(diverge, n, value)
        for i in range(ORDER):
            line = [ORDER * i + j for j in range(ORDER)]
            grads = along_line(derivative, [node(physical, n) for n in line])
            flux = []
            for n, value in zip(line, grads):
                put(grad_z.at[f], n, value)
                flux.append(node(weight, n) * value)
            for n, value in zip(line, along_line(derivative.T, flux)):
                put(diverge, n, node(diverge, n) + value)

    def stress(f, n, q):
        value = node(weight, n) * node(azimuth.at[f], n) if q else node(diverge, n)
        return value.astype(jnp.bfloat16)

    def to_coefficients(f, group_batches, found):
        spreads = []
        for batch in group_batches:
            entries = [entry for part in batch for entry in part]
            spreads.append(mm_nt(jnp.concatenate([stress(f, n, q) for n, q in entries], axis=0), wide[...]))
        cos, sin = turn[:tiles, :], turn[tiles:, :]
        for batch, spread in zip(group_batches, spreads):
            turned = {}
            for at, entry in enumerate(entry for part in batch for entry in part):
                re = spot(spread, 0, at * tiles, tiles)
                im = spot(spread, 1, at * tiles, tiles)
                turned[entry] = jnp.concatenate([re * cos + im * sin, im * cos - re * sin], axis=0).astype(
                    jnp.bfloat16
                )
            rhs = jnp.concatenate([stacked([turned[entry] for entry in part]) for part in batch], axis=1)
            back = mm(last_blocks[: max(len(part) for part in batch) * tiles, :], rhs)
            for b, part in enumerate(batch):
                for v, entry in enumerate(part):
                    found[entry] = spot(back, b, v * tiles, tiles)

    fields = ((disp_fwd, prev_fwd, next_fwd), (disp_adj, prev_adj, next_adj))
    for f, (disp, _, _) in enumerate(fields):
        if f == 0:
            for copy in small[2:6]:
                copy.wait()
            fetches[0].wait()
            fetches[1].wait()
            for copy in fetches[2:]:
                copy.start()
            first_blocks[...] = blocks_of(first[...], group)
            last_blocks[...] = blocks_of(last[...], group)
        else:
            fetches[2].wait()
        to_samples(f, disp, batches[0])
        to_samples(f, disp, batches[1])
        if f == 0:
            weights()
        found = {}
        mix(f)
        to_coefficients(f, back_batches[1] + back_batches[0], found)
        for n in range(nodes):
            div, phi = found[n, 0], found[n, 1]
            scale = ratio[n * half : (n + 1) * half, :]
            stiff[f, n, :half, :] = kept * div[:half] + scale * phi[half:]
            stiff[f, n, half:, :] = kept * div[half:] - scale * phi[:half]
        if f == 0:
            for copy in small[6:]:
                copy.wait()
            pl.semaphore_wait(barrier, sum(here.astype(jnp.int32) for here, _ in links))
        for side in range(4):
            lists = blk_nodes if side < 2 else band_nodes
            for s in range(side_slots[side]):
                send[f, side_start[side] + s] = stiff[f, lists[0, 0, side % 2, s]]

            @pl.when(early[side])
            def _():
                transfer(f, side).start()

    def follow(f):
        for side in range(2):

            @pl.when(late[side])
            def _():
                transfer(f, side).start()

    follow(0)
    follow(1)
    fetches[3].wait()
    for g in range(0, nodes, group):
        part = list(range(g, min(g + group, nodes)))
        products = [
            quad[n]
            * (
                node(grad_s.at[0], n) * node(grad_s.at[1], n)
                + node(grad_z.at[0], n) * node(grad_z.at[1], n)
                + node(azimuth.at[0], n) * node(azimuth.at[1], n)
            )
            for n in part
        ]
        turned = stacked(products).T
        spread = swap_granules([turned[h * tiles : (h + 1) * tiles, :] for h in range(group)], tiles)
        for n, value in zip(part, spread):
            put(kernel_out, n, node(kernel_in, n) - value)

    fetches[4].wait()
    fetches[5].wait()
    for f, (disp, prev, out) in enumerate(fields):
        for n in range(nodes):
            now = node(disp, n)
            value = now + now - node(prev, n) - step_scale[0, 0, n] * stiff[f, n]
            out[n * tiles : (n + 1) * tiles, :] = kept2 * value

    owners = [
        jnp.where(s < counts[0, 0, side], (blk_nodes, band_nodes)[side // 2][0, 0, side % 2, s], -1)
        for side in range(4)
        for s in range(side_slots[side])
    ]
    slot_of = []
    for n in range(nodes):
        found = jnp.int32(slots)
        for s, owner in enumerate(owners):
            found = jnp.where(owner == n, s, found)
        slot_of.append(found)

    for f, (_, _, out) in enumerate(fields):
        for side in range(4):

            @pl.when(links[side][0])
            def _():
                arrival(f, side).wait_recv()

        for n in range(nodes):
            out[n * tiles : (n + 1) * tiles, :] -= kept2 * step_scale[0, 0, n] * recv[f][slot_of[n]]
    for f in range(2):
        for side in range(4):

            @pl.when(links[side][0])
            def _():
                transfer(f, side).wait_send()


def deliver(one, two, three, one_out, two_out, three_out, sems):
    copies = [
        pltpu.make_async_copy(source, target, sems.at[i])
        for i, (source, target) in enumerate(((one, one_out), (two, two_out), (three, three_out)))
    ]
    for copy in copies:
        copy.start()
    for copy in copies:
        copy.wait()


def per_device(
    blk_total,
    band_total,
    disp_fwd,
    prev_fwd,
    disp_adj,
    prev_adj,
    modulus,
    radius,
    step_scale,
    kernel_in,
    buckets,
    halo_count,
    blk_nodes,
    band_nodes,
):
    nodes, coeff_len = disp_fwd.shape[2:]
    tiles = coeff_len // LANES
    slots = 2 * (blk_nodes.shape[-1] + band_nodes.shape[-1])
    first, last, wide, turn = stage_tables(tiles)
    hbm = pl.BlockSpec(memory_space=pltpu.HBM)
    vmem = pl.BlockSpec(memory_space=pltpu.VMEM)
    flat = (nodes * tiles, LANES)
    out = jax.ShapeDtypeStruct(flat, jnp.float32)
    outs = pl.pallas_call(
        functools.partial(kernel, blk_total, band_total, nodes, tiles),
        out_shape=(pltpu.VMEM(flat, jnp.float32),) * 3,
        in_specs=[hbm] * 16,
        out_specs=(vmem,) * 3,
        scratch_shapes=[
            pltpu.VMEM((6, *flat), jnp.float32),
            pltpu.VMEM(radius.shape, jnp.float32),
            pltpu.VMEM(buckets.shape, jnp.int32),
            pltpu.SMEM(step_scale.shape, jnp.float32),
            pltpu.SMEM(halo_count.shape, jnp.int32),
            pltpu.SMEM(blk_nodes.shape, jnp.int32),
            pltpu.SMEM(band_nodes.shape, jnp.int32),
            pltpu.VMEM(first.shape, jnp.bfloat16),
            pltpu.VMEM(last.shape, jnp.bfloat16),
            pltpu.VMEM(wide.shape, jnp.bfloat16),
            pltpu.VMEM(turn.shape, jnp.float32),
            pltpu.VMEM((2 * LANES, LANES), jnp.bfloat16),
            pltpu.VMEM((LANES, 2 * LANES), jnp.bfloat16),
            pltpu.VMEM((nodes * tiles // 2, LANES), jnp.float32),
            pltpu.VMEM(flat, jnp.float32),
            pltpu.VMEM(flat, jnp.float32),
            pltpu.VMEM((2, *flat), jnp.float32),
            pltpu.VMEM((2, *flat), jnp.float32),
            pltpu.VMEM((2, *flat), jnp.float32),
            pltpu.VMEM(flat, jnp.float32),
            pltpu.VMEM((2, nodes, tiles, LANES), jnp.float32),
            pltpu.VMEM((2, slots, tiles, LANES), jnp.float32),
            pltpu.VMEM((slots + 1, tiles, LANES), jnp.float32),
            pltpu.VMEM((slots + 1, tiles, LANES), jnp.float32),
            pltpu.SemaphoreType.DMA((6,)),
            pltpu.SemaphoreType.DMA((10,)),
            pltpu.SemaphoreType.DMA((2, 4)),
            pltpu.SemaphoreType.DMA((2, 4)),
        ],
        compiler_params=pltpu.CompilerParams(
            collective_id=0,
            has_side_effects=True,
            vmem_limit_bytes=67043328 - 3 * 4 * nodes * coeff_len - 40 * 1024,
        ),
    )(
        disp_fwd.reshape(flat),
        modulus.reshape(flat),
        disp_adj.reshape(flat),
        prev_fwd.reshape(flat),
        prev_adj.reshape(flat),
        kernel_in.reshape(flat),
        radius,
        buckets,
        step_scale,
        halo_count,
        blk_nodes,
        band_nodes,
        jnp.asarray(first),
        jnp.asarray(last),
        jnp.asarray(wide),
        jnp.asarray(turn),
    )
    outs = pl.pallas_call(
        deliver,
        out_shape=(out, out, out),
        in_specs=[vmem] * 3,
        out_specs=(hbm,) * 3,
        scratch_shapes=[pltpu.SemaphoreType.DMA((3,))],
        compiler_params=pltpu.CompilerParams(vmem_limit_bytes=4 * 1024 * 1024),
    )(*outs)
    return tuple(value.reshape(disp_fwd.shape) for value in outs)


def solution(mesh):
    wide = P("blk", "band", None, None)
    line = P("blk", "band", None)
    in_specs = (wide,) * 5 + (line, line, wide, P("blk", "band"), line, wide, wide)
    return jax.shard_map(
        functools.partial(per_device, mesh.shape["blk"], mesh.shape["band"]),
        mesh=mesh,
        in_specs=in_specs,
        out_specs=(wide,) * 3,
        check_vma=False,
    )
```

```python
import functools
import math

import jax
import jax.numpy as jnp
import ml_dtypes
import numpy as np
from jax import lax
from jax.experimental import pallas as pl
from jax.experimental.pallas import tpu as pltpu
from jax.sharding import PartitionSpec as P

MESH = pl.DeviceIdType.MESH
LANES = 128
ORDER = 5


def gll_tables():
    inner_root = math.sqrt(3.0 / 7.0)
    points = np.array([-1.0, -inner_root, 0.0, inner_root, 1.0])
    weights = np.array([0.1, 49.0 / 90.0, 32.0 / 45.0, 49.0 / 90.0, 0.1])
    legendre = (35.0 * points**4 - 30.0 * points**2 + 3.0) / 8.0
    derivative = np.zeros((5, 5))
    for target in range(5):
        for source in range(5):
            if target != source:
                derivative[target, source] = (
                    legendre[target] / legendre[source] / (points[target] - points[source])
                )
    derivative[0, 0] = -5.0
    derivative[4, 4] = 5.0
    return derivative.astype(np.float32), np.outer(weights, weights).astype(np.float32)


def rounded(value):
    return np.asarray(value, np.float32).astype(ml_dtypes.bfloat16)


def best_scale(value):
    levels = np.unique(np.round(np.abs(value), 12))
    factors = 1.0 + np.arange(10000) / 10000.0
    scaled = factors[:, None] * levels[None]
    loss = ((rounded(scaled).astype(np.float64) - scaled) ** 2).sum(axis=1) / factors**2
    return float(factors[np.argmin(loss)])


def stage_tables(tiles):
    total = tiles * LANES
    group = LANES // tiles
    angle = 2.0 * math.pi * np.outer(np.arange(tiles), np.arange(tiles // 2)) / tiles
    cos, sin = np.cos(angle), np.sin(angle)
    fold = np.block([[cos, -sin], [sin, cos]])
    kb = (np.arange(tiles)[None] * group + np.arange(group)[:, None]).reshape(-1)
    angle = 2.0 * math.pi * ((kb[:, None] * np.arange(LANES)[None]) % LANES) / LANES
    wide = np.concatenate([np.cos(angle), -np.sin(angle)], axis=1) * math.sqrt(2.0 / total)
    angle = 2.0 * math.pi * np.outer(np.arange(tiles), np.arange(LANES)) / total
    turn = np.concatenate([np.cos(angle), np.sin(angle)])
    fold_scale, wide_scale = best_scale(fold), best_scale(wide)
    first = rounded(np.tile(fold * fold_scale, (1, group)))
    last = rounded(np.tile(fold.T * fold_scale, (1, group)))
    turn = (turn / (fold_scale * wide_scale)).astype(np.float32)
    return first, last, rounded(wide.T * wide_scale), turn


def mm(lhs, rhs):
    return jnp.dot(lhs, rhs, preferred_element_type=jnp.float32)


def mm_nt(lhs, rhs):
    return lax.dot_general(lhs, rhs, (((1,), (1,)), ((), ())), preferred_element_type=jnp.float32)


def blocks_of(tile, group):
    rows, columns = tile.shape
    lane = lax.broadcasted_iota(jnp.int32, tile.shape, 1) // (columns // group)
    value = tile.astype(jnp.float32)
    parts = [jnp.where(lane == v, value, 0.0).astype(jnp.bfloat16) for v in range(group)]
    return jnp.concatenate(parts, axis=0)


def swap_granules(parts, tiles):
    parts = list(parts)
    lane = lax.broadcasted_iota(jnp.int32, parts[0].shape, 1)
    bit = len(parts) // 2
    while bit:
        upper = ((lane // tiles) & bit) != 0
        for a in range(len(parts)):
            if not a & bit:
                one, two = parts[a], parts[a | bit]
                parts[a] = jnp.where(upper, pltpu.roll(two, bit * tiles, 1), one)
                parts[a | bit] = jnp.where(upper, two, pltpu.roll(one, LANES - bit * tiles, 1))
        bit //= 2
    return parts


def along_line(table, line):
    sum0, dif0 = line[0] + line[4], line[0] - line[4]
    sum1, dif1 = line[1] + line[3], line[1] - line[3]
    out = [None] * 5
    for i in range(2):
        even = (
            float(table[i, 0] + table[i, 4]) / 2 * sum0
            + float(table[i, 1] + table[i, 3]) / 2 * sum1
            + float(table[i, 2]) * line[2]
        )
        odd = float(table[i, 0] - table[i, 4]) / 2 * dif0 + float(table[i, 1] - table[i, 3]) / 2 * dif1
        out[i], out[4 - i] = odd + even, odd - even
    out[2] = float(table[2, 0]) * dif0 + float(table[2, 1]) * dif1
    return out


def kernel(
    blk_total,
    band_total,
    nodes,
    tiles,
    disp_fwd_hbm,
    modulus_hbm,
    disp_adj_hbm,
    prev_fwd_hbm,
    prev_adj_hbm,
    kernel_in_hbm,
    radius_hbm,
    bucket_hbm,
    step_hbm,
    counts_hbm,
    blk_nodes_hbm,
    band_nodes_hbm,
    first_hbm,
    last_hbm,
    wide_hbm,
    turn_hbm,
    next_fwd,
    next_adj,
    kernel_out,
    held,
    radius,
    bucket,
    step_scale,
    counts,
    blk_nodes,
    band_nodes,
    first,
    last,
    wide,
    turn,
    first_blocks,
    last_blocks,
    ratio,
    weight,
    physical,
    azimuth,
    grad_s,
    grad_z,
    diverge,
    stiff,
    send,
    recv_fwd,
    recv_adj,
    held_sem,
    small_sem,
    send_sem,
    recv_sem,
):
    group = LANES // tiles
    half = tiles // 2
    recv = (recv_fwd, recv_adj)
    side_slots = [blk_nodes.shape[-1]] * 2 + [band_nodes.shape[-1]] * 2
    side_start = [sum(side_slots[:side]) for side in range(4)]
    slots = sum(side_slots)
    derivative, quadrature = gll_tables()
    quad = [float(value) for value in quadrature.reshape(-1)]

    def fetch(i, source, target, sems):
        return pltpu.make_async_copy(source, target, sems.at[i])

    sources = (disp_fwd_hbm, modulus_hbm, disp_adj_hbm, kernel_in_hbm, prev_fwd_hbm, prev_adj_hbm)
    fetches = [fetch(i, source, held.at[i], held_sem) for i, source in enumerate(sources)]
    disp_fwd, modulus, disp_adj, kernel_in, prev_fwd, prev_adj = (held.at[i] for i in range(6))
    small = [
        fetch(i, source, target, small_sem)
        for i, (source, target) in enumerate(
            (
                (radius_hbm, radius),
                (bucket_hbm, bucket),
                (first_hbm, first),
                (last_hbm, last),
                (turn_hbm, turn),
                (wide_hbm, wide),
                (step_hbm, step_scale),
                (counts_hbm, counts),
                (blk_nodes_hbm, blk_nodes),
                (band_nodes_hbm, band_nodes),
            )
        )
    ]
    small[0].start()
    small[1].start()
    fetches[0].start()
    for copy in small[2:6]:
        copy.start()
    fetches[1].start()
    for copy in small[6:]:
        copy.start()

    blk = lax.axis_index("blk")
    band = lax.axis_index("band")
    links = [
        (blk > 0, (blk - 1, band)),
        (blk < blk_total - 1, (blk + 1, band)),
        (band > 0, (blk, band - 1)),
        (band < band_total - 1, (blk, band + 1)),
    ]
    early = [links[0][0], links[1][0] & (blk != 1), links[2][0], links[3][0]]
    late = [blk < 0, links[1][0] & (blk == 1)]
    barrier = pltpu.get_barrier_semaphore()
    for here, peer in links:

        @pl.when(here)
        def _():
            pl.semaphore_signal(barrier, inc=1, device_id=peer, device_id_type=MESH)

    def rows(side):
        return pl.ds(side_start[side], side_slots[side])

    def transfer(f, side):
        return pltpu.make_async_remote_copy(
            src_ref=send.at[f, rows(side)],
            dst_ref=recv[f].at[rows(side ^ 1)],
            send_sem=send_sem.at[f, side],
            recv_sem=recv_sem.at[f, side ^ 1],
            device_id=links[side][1],
            device_id_type=MESH,
        )

    def arrival(f, side):
        return pltpu.make_async_remote_copy(
            src_ref=send.at[f, rows(side)],
            dst_ref=recv[f].at[rows(side)],
            send_sem=send_sem.at[f, side],
            recv_sem=recv_sem.at[f, side],
            device_id=links[side][1],
            device_id_type=MESH,
        )

    for side in range(4):

        @pl.when(jnp.logical_not(links[side][0]))
        def _():
            for ref in recv:
                ref[rows(side)] = jnp.zeros((side_slots[side], tiles, LANES), jnp.float32)

    for ref in recv:
        ref[slots] = jnp.zeros((tiles, LANES), jnp.float32)

    small[0].wait()
    small[1].wait()
    level = bucket[...]
    orders = half * LANES
    tops = [max(orders // 64, 1), max(orders // 16, 1), max(orders // 4, 1), orders]
    limit = jnp.where(
        level == 0, tops[0], jnp.where(level == 1, tops[1], jnp.where(level == 2, tops[2], tops[3]))
    )
    m = lax.broadcasted_iota(jnp.int32, (half, LANES), 0) * LANES + lax.broadcasted_iota(
        jnp.int32, (half, LANES), 1
    )
    kept = (m < limit).astype(jnp.float32)
    kept_m = m.astype(jnp.float32) * kept
    kept2 = jnp.concatenate([kept, kept], axis=0)
    inv_radius = 1.0 / radius[0]
    for n in range(nodes):
        ratio[n * half : (n + 1) * half, :] = kept_m * inv_radius[:, n : n + 1]

    def node(ref, n):
        return ref[n * tiles : (n + 1) * tiles, :]

    def put(ref, n, value):
        ref[n * tiles : (n + 1) * tiles, :] = value

    whole = nodes // group * group
    blocks = [[[(n, q) for n in range(g, g + group)] for g in range(0, whole, group)] for q in range(2)]
    spare = [(n, q) for n in range(whole, nodes) for q in range(2)]
    blocks[0] += [spare[g : g + group] for g in range(0, len(spare), group)]
    batches = [[[part] for part in side] for side in blocks]
    back_batches = [[[part] for part in side] for side in blocks]

    def stacked(parts):
        parts = parts + [jnp.zeros(parts[0].shape, parts[0].dtype)] * (group - len(parts))
        return jnp.concatenate(parts, axis=0)

    def spot(result, b, at, size):
        return result[at : at + size, b * LANES : (b + 1) * LANES]

    def coefficients(disp, n, q):
        value = node(disp, n)
        if q == 0:
            return (value * kept2).astype(jnp.bfloat16)
        scale = ratio[n * half : (n + 1) * half, :]
        return jnp.concatenate([value[half:] * -scale, value[:half] * scale], axis=0).astype(jnp.bfloat16)

    def to_samples(f, disp, group_batches):
        folds = []
        for batch in group_batches:
            rhs = jnp.concatenate(
                [stacked([coefficients(disp, n, q) for n, q in part]) for part in batch], axis=1
            )
            folds.append(mm(first_blocks[: max(len(part) for part in batch) * 2 * tiles, :], rhs))
        cos, sin = turn[:tiles, :], turn[tiles:, :]
        for batch, folded in zip(group_batches, folds):
            turned = []
            for b, part in enumerate(batch):
                for v in range(len(part)):
                    re = spot(folded, b, v * 2 * tiles, tiles)
                    im = spot(folded, b, (v * 2 + 1) * tiles, tiles)
                    turned.append(
                        jnp.concatenate([re * cos - im * sin, re * sin + im * cos], axis=1).astype(jnp.bfloat16)
                    )
            result = mm(jnp.concatenate(turned, axis=0), wide[...])
            for at, (n, q) in enumerate(entry for part in batch for entry in part):
                put((physical, azimuth.at[f])[q], n, spot(result, 0, at * tiles, tiles))

    def weights():
        for g in range(0, nodes, group):
            part = list(range(g, min(g + group, nodes)))
            parts = [node(modulus, n) for n in part]
            parts += [jnp.zeros((tiles, LANES), jnp.float32)] * (group - len(part))
            turned = jnp.concatenate(swap_granules(parts, tiles), axis=0).T
            for v, n in enumerate(part):
                put(weight, n, quad[n] * turned[v * tiles : (v + 1) * tiles, :])

    def mix(f):
        for j in range(ORDER):
            line = [ORDER * i + j for i in range(ORDER)]
            grads = along_line(derivative, [node(physical, n) for n in line])
            flux = []
            for n, value in zip(line, grads):
                put(grad_s.at[f], n, value)
                flux.append(node(weight, n) * value)
            for n, value in zip(line, along_line(derivative.T, flux)):
                put(diverge, n, value)
        for i in range(ORDER):
            line = [ORDER * i + j for j in range(ORDER)]
            grads = along_line(derivative, [node(physical, n) for n in line])
            flux = []
            for n, value in zip(line, grads):
                put(grad_z.at[f], n, value)
                flux.append(node(weight, n) * value)
            for n, value in zip(line, along_line(derivative.T, flux)):
                put(diverge, n, node(diverge, n) + value)

    def stress(f, n, q):
        value = node(weight, n) * node(azimuth.at[f], n) if q else node(diverge, n)
        return value.astype(jnp.bfloat16)

    def to_coefficients(f, group_batches, found):
        spreads = []
        for batch in group_batches:
            entries = [entry for part in batch for entry in part]
            spreads.append(mm_nt(jnp.concatenate([stress(f, n, q) for n, q in entries], axis=0), wide[...]))
        cos, sin = turn[:tiles, :], turn[tiles:, :]
        for batch, spread in zip(group_batches, spreads):
            turned = {}
            for at, entry in enumerate(entry for part in batch for entry in part):
                re = spot(spread, 0, at * tiles, tiles)
                im = spot(spread, 1, at * tiles, tiles)
                turned[entry] = jnp.concatenate([re * cos + im * sin, im * cos - re * sin], axis=0).astype(
                    jnp.bfloat16
                )
            rhs = jnp.concatenate([stacked([turned[entry] for entry in part]) for part in batch], axis=1)
            back = mm(last_blocks[: max(len(part) for part in batch) * tiles, :], rhs)
            for b, part in enumerate(batch):
                for v, entry in enumerate(part):
                    found[entry] = spot(back, b, v * tiles, tiles)

    fields = ((disp_fwd, prev_fwd, next_fwd), (disp_adj, prev_adj, next_adj))
    for f, (disp, _, _) in enumerate(fields):
        if f == 0:
            for copy in small[2:6]:
                copy.wait()
            fetches[0].wait()
            fetches[1].wait()
            for copy in fetches[2:]:
                copy.start()
            first_blocks[...] = blocks_of(first[...], group)
            last_blocks[...] = blocks_of(last[...], group)
        else:
            fetches[2].wait()
        to_samples(f, disp, batches[0] + batches[1])
        if f == 0:
            weights()
        found = {}
        mix(f)
        to_coefficients(f, back_batches[1] + back_batches[0], found)
        for n in range(nodes):
            div, phi = found[n, 0], found[n, 1]
            scale = ratio[n * half : (n + 1) * half, :]
            stiff[f, n, :half, :] = kept * div[:half] + scale * phi[half:]
            stiff[f, n, half:, :] = kept * div[half:] - scale * phi[:half]
        if f == 0:
            for copy in small[6:]:
                copy.wait()
            pl.semaphore_wait(barrier, sum(here.astype(jnp.int32) for here, _ in links))
        for side in range(4):
            lists = blk_nodes if side < 2 else band_nodes
            for s in range(side_slots[side]):
                send[f, side_start[side] + s] = stiff[f, lists[0, 0, side % 2, s]]

            @pl.when(early[side])
            def _():
                transfer(f, side).start()

    def follow(f):
        for side in range(2):

            @pl.when(late[side])
            def _():
                transfer(f, side).start()

    follow(0)
    follow(1)
    fetches[3].wait()
    for g in range(0, nodes, group):
        part = list(range(g, min(g + group, nodes)))
        products = [
            quad[n]
            * (
                node(grad_s.at[0], n) * node(grad_s.at[1], n)
                + node(grad_z.at[0], n) * node(grad_z.at[1], n)
                + node(azimuth.at[0], n) * node(azimuth.at[1], n)
            )
            for n in part
        ]
        turned = stacked(products).T
        spread = swap_granules([turned[h * tiles : (h + 1) * tiles, :] for h in range(group)], tiles)
        for n, value in zip(part, spread):
            put(kernel_out, n, node(kernel_in, n) - value)

    fetches[4].wait()
    fetches[5].wait()
    for f, (disp, prev, out) in enumerate(fields):
        for n in range(nodes):
            now = node(disp, n)
            value = now + now - node(prev, n) - step_scale[0, 0, n] * stiff[f, n]
            out[n * tiles : (n + 1) * tiles, :] = kept2 * value

    owners = [
        jnp.where(s < counts[0, 0, side], (blk_nodes, band_nodes)[side // 2][0, 0, side % 2, s], -1)
        for side in range(4)
        for s in range(side_slots[side])
    ]
    slot_of = []
    for n in range(nodes):
        found = jnp.int32(slots)
        for s, owner in enumerate(owners):
            found = jnp.where(owner == n, s, found)
        slot_of.append(found)

    for f, (_, _, out) in enumerate(fields):
        for side in range(4):

            @pl.when(links[side][0])
            def _():
                arrival(f, side).wait_recv()

        for n in range(nodes):
            out[n * tiles : (n + 1) * tiles, :] -= kept2 * step_scale[0, 0, n] * recv[f][slot_of[n]]
    for f in range(2):
        for side in range(4):

            @pl.when(links[side][0])
            def _():
                transfer(f, side).wait_send()


def deliver(one, two, three, one_out, two_out, three_out, sems):
    copies = [
        pltpu.make_async_copy(source, target, sems.at[i])
        for i, (source, target) in enumerate(((one, one_out), (two, two_out), (three, three_out)))
    ]
    for copy in copies:
        copy.start()
    for copy in copies:
        copy.wait()


def per_device(
    blk_total,
    band_total,
    disp_fwd,
    prev_fwd,
    disp_adj,
    prev_adj,
    modulus,
    radius,
    step_scale,
    kernel_in,
    buckets,
    halo_count,
    blk_nodes,
    band_nodes,
):
    nodes, coeff_len = disp_fwd.shape[2:]
    tiles = coeff_len // LANES
    slots = 2 * (blk_nodes.shape[-1] + band_nodes.shape[-1])
    first, last, wide, turn = stage_tables(tiles)
    hbm = pl.BlockSpec(memory_space=pltpu.HBM)
    vmem = pl.BlockSpec(memory_space=pltpu.VMEM)
    flat = (nodes * tiles, LANES)
    out = jax.ShapeDtypeStruct(flat, jnp.float32)
    outs = pl.pallas_call(
        functools.partial(kernel, blk_total, band_total, nodes, tiles),
        out_shape=(pltpu.VMEM(flat, jnp.float32),) * 3,
        in_specs=[hbm] * 16,
        out_specs=(vmem,) * 3,
        scratch_shapes=[
            pltpu.VMEM((6, *flat), jnp.float32),
            pltpu.VMEM(radius.shape, jnp.float32),
            pltpu.VMEM(buckets.shape, jnp.int32),
            pltpu.SMEM(step_scale.shape, jnp.float32),
            pltpu.SMEM(halo_count.shape, jnp.int32),
            pltpu.SMEM(blk_nodes.shape, jnp.int32),
            pltpu.SMEM(band_nodes.shape, jnp.int32),
            pltpu.VMEM(first.shape, jnp.bfloat16),
            pltpu.VMEM(last.shape, jnp.bfloat16),
            pltpu.VMEM(wide.shape, jnp.bfloat16),
            pltpu.VMEM(turn.shape, jnp.float32),
            pltpu.VMEM((2 * LANES, LANES), jnp.bfloat16),
            pltpu.VMEM((LANES, 2 * LANES), jnp.bfloat16),
            pltpu.VMEM((nodes * tiles // 2, LANES), jnp.float32),
            pltpu.VMEM(flat, jnp.float32),
            pltpu.VMEM(flat, jnp.float32),
            pltpu.VMEM((2, *flat), jnp.float32),
            pltpu.VMEM((2, *flat), jnp.float32),
            pltpu.VMEM((2, *flat), jnp.float32),
            pltpu.VMEM(flat, jnp.float32),
            pltpu.VMEM((2, nodes, tiles, LANES), jnp.float32),
            pltpu.VMEM((2, slots, tiles, LANES), jnp.float32),
            pltpu.VMEM((slots + 1, tiles, LANES), jnp.float32),
            pltpu.VMEM((slots + 1, tiles, LANES), jnp.float32),
            pltpu.SemaphoreType.DMA((6,)),
            pltpu.SemaphoreType.DMA((10,)),
            pltpu.SemaphoreType.DMA((2, 4)),
            pltpu.SemaphoreType.DMA((2, 4)),
        ],
        compiler_params=pltpu.CompilerParams(
            collective_id=0,
            has_side_effects=True,
            vmem_limit_bytes=67043328 - 3 * 4 * nodes * coeff_len - 40 * 1024,
        ),
    )(
        disp_fwd.reshape(flat),
        modulus.reshape(flat),
        disp_adj.reshape(flat),
        prev_fwd.reshape(flat),
        prev_adj.reshape(flat),
        kernel_in.reshape(flat),
        radius,
        buckets,
        step_scale,
        halo_count,
        blk_nodes,
        band_nodes,
        jnp.asarray(first),
        jnp.asarray(last),
        jnp.asarray(wide),
        jnp.asarray(turn),
    )
    outs = pl.pallas_call(
        deliver,
        out_shape=(out, out, out),
        in_specs=[vmem] * 3,
        out_specs=(hbm,) * 3,
        scratch_shapes=[pltpu.SemaphoreType.DMA((3,))],
        compiler_params=pltpu.CompilerParams(vmem_limit_bytes=4 * 1024 * 1024),
    )(*outs)
    return tuple(value.reshape(disp_fwd.shape) for value in outs)


def solution(mesh):
    wide = P("blk", "band", None, None)
    line = P("blk", "band", None)
    in_specs = (wide,) * 5 + (line, line, wide, P("blk", "band"), line, wide, wide)
    return jax.shard_map(
        functools.partial(per_device, mesh.shape["blk"], mesh.shape["band"]),
        mesh=mesh,
        in_specs=in_specs,
        out_specs=(wide,) * 3,
        check_vma=False,
    )
```
